256 devices in a mesh: groups: 2 (over y), px: 64 (over z, x), py: 2 (over core).
Axes of the slice: x: 4, y: 2, z: 16, core: 2. Of those that a mesh axis runs over, the one named last changes fastest.
The devices are a block of a 4x16x16 slice.
Arguments:
- field: bfloat16 [2, 20, 384, 192, 128], P('groups', None, 'px', 'py'), parts along dimension 0, may hold values from -6 to 6
- spectral_weight: bfloat16 [2, 20, 20, 1536, 96], P(None, None, None, ('py', 'px')), may hold values from -6 to 6
- pointwise_weight: bfloat16 [20, 20], replicated, may hold values from -1.25 to 1.25
- bias: float32 [20], replicated, may hold values from -3 to 3
Outputs:
- mixed_field: bfloat16 [2, 20, 384, 192, 128], P('groups', None, 'px', 'py'), parts along dimension 0
The draws below stay inside these ranges and needn't reach their ends.
There are 2 independent parts, one for each index of `groups`. The reference program is written for one: setup_inputs(seed, part) draws one part's arguments, and reference() takes and returns one part's arrays. A program takes and returns all parts, laid end to end along the dimension named above; an argument that names none is the same for every part. Nothing has to cross between parts.
All inputs are finite; a program needn't handle non-finite values.
Results may differ from the reference program's by a relative error of at most 0.001.
Values sent between devices are 32-bit elements; how exact they have to be, the bound alone decides.
No kernel may reach another device: no remote copies, remote signals or barrier semaphores. Data moves between devices by JAX's collectives and lax.ppermute only.
A program may use at most 128 MiB of HBM per device.

```python
import jax
import jax.numpy as jnp
from jax import lax

B = 1
C = 20
NX = 384
NY = 192
NZ = 128
MX = 96
MY = 48
MZ = 32


def block_scale(rng, shape, split, smallest, largest):
    loudness, own = 1.0, jax.random.fold_in(rng, 6)
    for axis_at, shards_of in split:
        steps = jnp.exp(jax.random.uniform(jax.random.fold_in(own, axis_at), (shards_of,), jnp.float32, smallest / len(split), largest / len(split)))
        loudness = loudness * jnp.repeat(steps, shape[axis_at] // shards_of).reshape([-1 if axis == axis_at else 1 for axis in range(len(shape))])
    return loudness


def centred(key, shape, deviation, bound, shards=(), kind=jnp.bfloat16):
    result = jax.random.normal(key, shape, jnp.float32) * deviation
    if len(shards) > 0:
        result = block_scale(key, shape, shards, -0.22, 0.18) * result
    return jnp.clip(result, min=-bound, max=bound).astype(kind)


def setup_inputs(seed: int = 0, part: int = 0) -> dict:
    arg_keys = jax.random.split(jax.random.key(seed), 5)
    part_keys = jax.random.split(jax.random.fold_in(arg_keys[4], part), 5)
    field = centred(part_keys[0], (B, C, NX, NY, NZ), 1.0, 6.0, ((2, 64), (3, 2)))
    spectral_weight = centred(arg_keys[1], (2, C, C, MZ * MY, MX), 0.9, 6.0, ((3, 128),))
    pointwise_weight = centred(arg_keys[2], (C, C), C ** -0.5, 1.25)
    bias = centred(arg_keys[3], (C,), 0.5, 3.0, (), jnp.float32)
    return dict(field=field, spectral_weight=spectral_weight, pointwise_weight=pointwise_weight, bias=bias)


def spread_axis(values, axis, length):
    kept = values.shape[axis]
    half = kept // 2
    lower = lax.slice_in_dim(values, 0, half, axis=axis)
    upper = lax.slice_in_dim(values, half, kept, axis=axis)
    shape = list(values.shape)
    shape[axis] = length - kept
    return jnp.concatenate([lower, jnp.zeros(shape, values.dtype), upper], axis)


def mix_modes(weight_part, values):
    return jnp.einsum("iozyx,izyx->ozyx", weight_part, values, precision=lax.Precision.HIGHEST)


def reference(field, spectral_weight, pointwise_weight, bias):
    weights = spectral_weight.astype(jnp.float32).reshape(2, C, C, MZ, MY, MX)
    results = []
    for sample in range(B):
        volume = field[sample]

        def forward(channel):
            spectrum = jnp.fft.rfftn(channel.astype(jnp.float32))
            spectrum = jnp.concatenate([spectrum[:MX // 2], spectrum[NX - MX // 2:]], 0)
            spectrum = jnp.concatenate([spectrum[:, :MY // 2], spectrum[:, NY - MY // 2:]], 1)
            spectrum = jnp.transpose(spectrum[:, :, :MZ], (2, 1, 0))
            return jnp.real(spectrum), jnp.imag(spectrum)

        real_in, imag_in = lax.map(forward, volume)
        real_out = mix_modes(weights[0], real_in) - mix_modes(weights[1], imag_in)
        imag_out = mix_modes(weights[0], imag_in) + mix_modes(weights[1], real_in)
        flat_volume = volume.reshape(C, -1)

        def inverse(inputs):
            channel_index, real_part, imag_part = inputs
            parts = []
            for values in (real_part, imag_part):
                values = jnp.transpose(values, (2, 1, 0))
                values = spread_axis(values, 0, NX)
                values = spread_axis(values, 1, NY)
                values = jnp.pad(values, ((0, 0), (0, 0), (0, NZ // 2 + 1 - MZ)))
                parts.append(values)
            spectral = jnp.fft.irfftn(lax.complex(parts[0], parts[1]), s=(NX, NY, NZ))
            column = lax.dynamic_slice_in_dim(pointwise_weight, channel_index, 1, 1).reshape(1, C)
            local_part = jnp.dot(column, flat_volume, preferred_element_type=jnp.float32).reshape(NX, NY, NZ)
            total = spectral + local_part + lax.dynamic_slice_in_dim(bias, channel_index, 1, 0)[0]
            return jax.nn.gelu(total).astype(jnp.bfloat16)

        results.append(lax.map(inverse, (jnp.arange(C, dtype=jnp.int32), real_out, imag_out)))
    return jnp.stack(results)
```

```python
import functools
import math

import jax
import jax.numpy as jnp
import numpy as np
from jax import lax
from jax.experimental import pallas as pl
from jax.experimental.pallas import tpu as pltpu
from jax.sharding import PartitionSpec as P

NX = 384
NY = 192
NZ = 128
MX = 96
MY = 48
MZ = 32

LANES = 128
QUAD = 4
Y_BLOCKS = 4
M = MY // Y_BLOCKS
MP = 16
HALF = 64
VMEM_LIMIT = 60 * 1024 * 1024


def kept(length, retained):
    index = np.arange(retained)
    return np.where(index < retained // 2, index, length - retained + index)


def angles(frequency, positions, length):
    return 2 * np.pi * ((frequency[:, None] * positions[None, :]) % length) / length


def halves(table):
    high = table.astype(np.float32).astype(jnp.bfloat16)
    low = (table - high.astype(np.float64)).astype(np.float32).astype(jnp.bfloat16)
    return np.stack([high, low])


def split(value):
    high = value.astype(jnp.bfloat16)
    low = (value - high.astype(jnp.float32)).astype(jnp.bfloat16)
    return high, low


def dot(a, b, contract=((1,), (0,))):
    return lax.dot_general(a, b, (contract, ((), ())), preferred_element_type=jnp.float32)


def z_order(y_devices):
    order = np.arange(MZ).reshape(y_devices, MZ // y_devices)
    return [np.concatenate([order[d], np.delete(order, d, 0).reshape(-1)]) for d in range(y_devices)]


def z_forward_table(y_devices):
    tables = []
    for kz in z_order(y_devices):
        angle = angles(kz, np.arange(NZ), NZ).T
        table = np.zeros((QUAD, NZ, 2, QUAD, MZ))
        for c in range(QUAD):
            table[c, :, 0, c] = np.cos(angle)
            table[c, :, 1, c] = -np.sin(angle)
        tables.append(halves(table.reshape(QUAD * NZ, 2 * QUAD * MZ)))
    return np.stack(tables)


def y_forward_table(y_devices):
    tables = []
    rows = NY // y_devices
    for d in range(y_devices):
        angle = angles(kept(NY, MY), d * rows + np.arange(rows), NY)
        table = np.zeros((2, Y_BLOCKS, MP, rows))
        table[0, :, :M] = np.cos(angle).reshape(Y_BLOCKS, M, rows)
        table[1, :, :M] = np.sin(angle).reshape(Y_BLOCKS, M, rows)
        tables.append(halves(table.reshape(2 * Y_BLOCKS * MP, rows)))
    return np.stack(tables)


def x_table():
    angle = angles(kept(NX, MX), np.arange(NX), NX).T
    table = np.zeros((NX, 2, LANES))
    table[:, 0, :MX] = np.cos(angle)
    table[:, 1, :MX] = np.sin(angle)
    return halves(table.reshape(NX, 2 * LANES))


def y_inverse_table(y_devices):
    tables = []
    rows = NY // y_devices
    for d in range(y_devices):
        angle = angles(kept(NY, MY), d * rows + np.arange(rows), NY).T
        table = np.zeros((2, rows, 2, Y_BLOCKS, MP))
        cosine = np.cos(angle).reshape(rows, Y_BLOCKS, M)
        sine = np.sin(angle).reshape(rows, Y_BLOCKS, M)
        table[0, :, 0, :, :M] = cosine
        table[0, :, 1, :, :M] = -sine
        table[1, :, 0, :, :M] = sine
        table[1, :, 1, :, :M] = cosine
        tables.append(halves(table.reshape(2 * rows, 2 * Y_BLOCKS * MP)))
    return np.stack(tables)


def z_inverse_table(y_devices):
    tables = []
    for kz in z_order(y_devices):
        angle = angles(kz, np.arange(NZ), NZ)
        weight = np.where(kz == 0, 1.0, 2.0)[:, None] / (NX * NY * NZ)
        table = np.zeros((2, QUAD, MZ, QUAD, NZ))
        for c in range(QUAD):
            table[0, c, :, c] = np.cos(angle) * weight
            table[1, c, :, c] = -np.sin(angle) * weight
        tables.append(halves(table.reshape(2 * QUAD * MZ, QUAD * NZ)))
    return np.stack(tables)


def forward_kernel(place, field, z_table, y_table, own, other, rows):
    x = pl.program_id(0)
    channels = field.shape[0]
    groups = channels // QUAD
    per_x = QUAD * MZ
    half = MZ // 2
    stride = Y_BLOCKS * own.shape[1]
    for g in range(groups):
        cells = jnp.concatenate([field[QUAD * g + c, 0] for c in range(QUAD)], 1)
        z_hat = dot(cells, z_table[0, 0]) + dot(cells, z_table[0, 1])
        high, low = split(z_hat)
        parts = dot(y_table[0, 0], high) + dot(y_table[0, 0], low) + dot(y_table[0, 1], high)
        size = Y_BLOCKS * MP
        real = parts[:size, :per_x] + parts[size:, per_x:]
        imag = parts[:size, per_x:] - parts[size:, :per_x]
        for block in range(Y_BLOCKS):
            for s, value in enumerate((real, imag)):
                rows[block, pl.ds(s * HALF + g * M, MP), :] = value[block * MP : (block + 1) * MP]
    del place
    own_rows = own.reshape(own.shape[0] * own.shape[1], LANES)
    other_rows = other.reshape(other.shape[0] * other.shape[1], LANES)
    for block in range(Y_BLOCKS):
        turned = rows[block, :LANES, :].T
        for c in range(QUAD):
            start = block * own.shape[1] + x * QUAD + c
            at = pl.ds(start, half, stride=stride)
            own_rows[at, :] = turned[c * MZ : c * MZ + half]
            other_rows[at, :] = turned[c * MZ + half : (c + 1) * MZ]


def forward(place, field, y_devices, x_devices):
    channels, x_local, y_local, _ = field.shape
    z_table, y_table = z_forward_table(y_devices), y_forward_table(y_devices)
    payload = jax.ShapeDtypeStruct((x_devices, x_local * QUAD, LANES), jnp.float32)
    whole = pl.BlockSpec(payload.shape, lambda x, p: (0, 0, 0))
    return pl.pallas_call(
        forward_kernel,
        out_shape=(payload, payload),
        grid_spec=pltpu.PrefetchScalarGridSpec(
            num_scalar_prefetch=1,
            grid=(x_local,),
            in_specs=[
                pl.BlockSpec((channels, 1, y_local, NZ), lambda x, p: (0, x, 0, 0)),
                pl.BlockSpec((1, *z_table.shape[1:]), lambda x, p: (p[0], 0, 0, 0)),
                pl.BlockSpec((1, *y_table.shape[1:]), lambda x, p: (p[0], 0, 0, 0)),
            ],
            out_specs=[whole, whole],
            scratch_shapes=[pltpu.VMEM((Y_BLOCKS, LANES + MP, LANES), jnp.float32)],
        ),
        compiler_params=pltpu.CompilerParams(
            dimension_semantics=("arbitrary",), vmem_limit_bytes=VMEM_LIMIT
        ),
        name="forward",
    )(place, field, jnp.asarray(z_table), jnp.asarray(y_table))


def mix_kernel(payload, weights, table, result, spectrum, mixed):
    channels = weights.shape[1]
    groups = channels // QUAD
    source = payload.reshape(payload.shape[0] * payload.shape[1], LANES)
    target = result.reshape(result.shape[0] * result.shape[1], LANES)
    for c in range(QUAD):
        high, low = split(source[pl.ds(c, NX, stride=QUAD), :])
        over_x = ((0,), (0,))
        parts = dot(high, table[0], over_x) + dot(low, table[0], over_x) + dot(high, table[1], over_x)
        spectrum[c, 0] = parts[:HALF, :LANES] + parts[HALF:, LANES:]
        spectrum[c, 1] = parts[HALF:, :LANES] - parts[:HALF, LANES:]
    outs = channels // 2
    for first in range(0, channels, outs):
        real = [jnp.zeros((MP, LANES), jnp.float32)] * outs
        imag = [jnp.zeros((MP, LANES), jnp.float32)] * outs
        for i in range(channels):
            g, c = i // QUAD, i % QUAD
            real_in = spectrum[c, 0, pl.ds(g * M, MP), :]
            imag_in = spectrum[c, 1, pl.ds(g * M, MP), :]
            for k in range(outs):
                w_real = weights[0, i, first + k].astype(jnp.float32)
                w_imag = weights[1, i, first + k].astype(jnp.float32)
                real[k] = real[k] + (w_real * real_in - w_imag * imag_in)
                imag[k] = imag[k] + (w_real * imag_in + w_imag * real_in)
        for k in range(outs):
            g, c = (first + k) // QUAD, (first + k) % QUAD
            upper = pl.ds(g * M, MP)
            lower = pl.ds(HALF + g * M, MP)
            mixed[c, upper, :LANES] = real[k]
            mixed[c, upper, LANES:] = -imag[k]
            mixed[c, lower, :LANES] = imag[k]
            mixed[c, lower, LANES:] = real[k]
    del groups
    for c in range(QUAD):
        high, low = split(mixed[c, :LANES, :])
        over_k = ((1,), (1,))
        back = dot(table[0], high, over_k) + dot(table[0], low, over_k) + dot(table[1], high, over_k)
        target[pl.ds(c, NX, stride=QUAD), :] = back


def mix(payload, weights):
    table = x_table()
    vmem = pl.BlockSpec(memory_space=pltpu.VMEM)
    return pl.pallas_call(
        mix_kernel,
        out_shape=jax.ShapeDtypeStruct(payload.shape, jnp.float32),
        in_specs=[vmem, vmem, vmem],
        out_specs=vmem,
        scratch_shapes=[
            pltpu.VMEM((QUAD, 2, HALF, LANES), jnp.float32),
            pltpu.VMEM((QUAD, LANES + MP, 2 * LANES), jnp.float32),
        ],
        compiler_params=pltpu.CompilerParams(vmem_limit_bytes=VMEM_LIMIT),
        name="mix",
    )(payload, weights, jnp.asarray(table))


def inverse_kernel(place, own, other, field, y_table, z_table, local, bias, out, rows, modes, total):
    del place
    x = pl.program_id(0)
    channels, _, y_local, _ = field.shape
    groups = channels // QUAD
    half = MZ // 2
    stride = Y_BLOCKS * own.shape[1]
    own_rows = own.reshape(own.shape[0] * own.shape[1], LANES)
    other_rows = other.reshape(other.shape[0] * other.shape[1], LANES)
    for block in range(Y_BLOCKS):
        for c in range(QUAD):
            start = block * own.shape[1] + x * QUAD + c
            at = pl.ds(start, half, stride=stride)
            rows[c * MZ : c * MZ + half] = own_rows[at, :]
            rows[c * MZ + half : (c + 1) * MZ] = other_rows[at, :]
        modes[block] = rows[...].T
    for g in range(groups):
        inputs = jnp.concatenate(
            [modes[block, pl.ds(s * HALF + g * M, MP), :] for s in range(2) for block in range(Y_BLOCKS)], 0
        )
        high, low = split(inputs)
        lines = dot(y_table[0, 0], high) + dot(y_table[0, 0], low) + dot(y_table[0, 1], high)
        lines = jnp.concatenate([lines[:y_local], lines[y_local:]], 1)
        high, low = split(lines)
        cells = dot(high, z_table[0, 0]) + dot(low, z_table[0, 0]) + dot(high, z_table[0, 1])
        for c in range(QUAD):
            total[QUAD * g + c] = cells[:, c * NZ : (c + 1) * NZ]
    step = MP
    for y in range(0, y_local, 2 * step):
        pair = [
            field[:, 0, y + j * step : y + (j + 1) * step, :].reshape(channels * step, NZ) for j in range(2)
        ]
        mixed = dot(local[...], jnp.concatenate(pair, 1))
        for o in range(channels):
            for j in range(2):
                at = slice(y + j * step, y + (j + 1) * step)
                value = mixed[o * step : (o + 1) * step, j * NZ : (j + 1) * NZ]
                value = value + total[o, at, :] + bias[o]
                inner = math.sqrt(2 / math.pi) * (value + 0.044715 * (value * value * value))
                out[o, 0, at, :] = (0.5 * value * (1.0 + jnp.tanh(inner))).astype(out.dtype)


def inverse(place, own, other, field, local, bias, y_devices):
    channels, x_local, y_local, _ = field.shape
    z_table, y_table = z_inverse_table(y_devices), y_inverse_table(y_devices)
    whole = pl.BlockSpec(own.shape, lambda x, p: (0, 0, 0))
    cells = pl.BlockSpec((channels, 1, y_local, NZ), lambda x, p: (0, x, 0, 0))
    return pl.pallas_call(
        inverse_kernel,
        out_shape=jax.ShapeDtypeStruct(field.shape, field.dtype),
        grid_spec=pltpu.PrefetchScalarGridSpec(
            num_scalar_prefetch=1,
            grid=(x_local,),
            in_specs=[
                whole,
                whole,
                cells,
                pl.BlockSpec((1, *y_table.shape[1:]), lambda x, p: (p[0], 0, 0, 0)),
                pl.BlockSpec((1, *z_table.shape[1:]), lambda x, p: (p[0], 0, 0, 0)),
                pl.BlockSpec(local.shape, lambda x, p: (0, 0)),
                pl.BlockSpec(memory_space=pltpu.SMEM),
            ],
            out_specs=cells,
            scratch_shapes=[
                pltpu.VMEM((LANES, LANES), jnp.float32),
                pltpu.VMEM((Y_BLOCKS, LANES, LANES), jnp.float32),
                pltpu.VMEM((channels, y_local, NZ), jnp.float32),
            ],
        ),
        compiler_params=pltpu.CompilerParams(
            dimension_semantics=("arbitrary",), vmem_limit_bytes=VMEM_LIMIT
        ),
        name="inverse",
    )(place, own, other, field, jnp.asarray(y_table), jnp.asarray(z_table), local, bias)


def spread_weights(spectral_weight):
    m, k = spectral_weight.shape[3:]
    return jnp.pad(spectral_weight, ((0, 0), (0, 0), (0, 0), (0, MP - m), (0, LANES - k)))


def local_matrix(pointwise_weight):
    channels = pointwise_weight.shape[0]
    eye = jnp.eye(MP, dtype=pointwise_weight.dtype)
    matrix = pointwise_weight.T[:, None, :, None] * eye[None, :, None, :]
    return matrix.reshape(channels * MP, channels * MP)


def swapped(x, axis):
    devices = lax.axis_size(axis)
    return lax.ppermute(x, axis, [(d, (d + 1) % devices) for d in range(devices)])


def per_device(field, spectral_weight, pointwise_weight, bias):
    y_devices, x_devices = lax.axis_size("py"), lax.axis_size("px")
    place = lax.axis_index("py").astype(jnp.int32).reshape(1)
    cells = field[0]
    weights = spread_weights(spectral_weight)
    local = local_matrix(pointwise_weight)
    own, other = forward(place, cells, y_devices, x_devices)
    payload = own + swapped(other, "py")
    received = lax.all_to_all(payload, "px", 0, 0, tiled=True)
    result = mix(received, weights)
    own = lax.all_to_all(result, "px", 0, 0, tiled=True)
    other = swapped(own, "py")
    return inverse(place, own, other, cells, local, bias, y_devices)[None]


def solution(mesh):
    in_specs = (
        P("groups", None, "px", "py", None),
        P(None, None, None, ("py", "px"), None),
        P(),
        P(),
    )
    out_specs = P("groups", None, "px", "py", None)
    return jax.shard_map(per_device, mesh=mesh, in_specs=in_specs, out_specs=out_specs, check_vma=False)
```

```python
import functools
import math

import jax
import jax.numpy as jnp
import numpy as np
from jax import lax
from jax.experimental import pallas as pl
from jax.experimental.pallas import tpu as pltpu
from jax.sharding import PartitionSpec as P

NX = 384
NY = 192
NZ = 128
MX = 96
MY = 48
MZ = 32

LANES = 128
QUAD = 4
Y_BLOCKS = 4
M = MY // Y_BLOCKS
MP = 16
HALF = 64
X_STEP = 2
MIB = 1024 * 1024


def kept(length, retained):
    index = np.arange(retained)
    return np.where(index < retained // 2, index, length - retained + index)


def angles(frequency, positions, length):
    return 2 * np.pi * ((frequency[:, None] * positions[None, :]) % length) / length


def halves(table):
    high = table.astype(np.float32).astype(jnp.bfloat16)
    low = (table - high.astype(np.float64)).astype(np.float32).astype(jnp.bfloat16)
    return np.stack([high, low])


def split(value):
    high = value.astype(jnp.bfloat16)
    low = (value - high.astype(jnp.float32)).astype(jnp.bfloat16)
    return high, low


def dot(a, b, contract=((1,), (0,))):
    return lax.dot_general(a, b, (contract, ((), ())), preferred_element_type=jnp.float32)


def z_order(y_devices):
    order = np.arange(MZ).reshape(y_devices, MZ // y_devices)
    return [np.concatenate([order[d], np.delete(order, d, 0).reshape(-1)]) for d in range(y_devices)]


def z_forward_table(y_devices):
    tables = []
    for kz in z_order(y_devices):
        angle = np.tile(angles(kz, np.arange(NZ), NZ).T, (1, QUAD))
        tables.append(halves(np.concatenate([np.cos(angle), -np.sin(angle)], 1)))
    return np.stack(tables)


def stacked(table):
    high, low = halves(table)
    return np.concatenate([np.concatenate([high, high], 1), np.concatenate([low, np.zeros_like(low)], 1)], 0)


def y_forward_table(y_devices):
    tables = []
    rows = NY // y_devices
    for d in range(y_devices):
        angle = angles(kept(NY, MY), d * rows + np.arange(rows), NY)
        table = np.zeros((2, Y_BLOCKS, MP, rows))
        table[0, :, :M] = np.cos(angle).reshape(Y_BLOCKS, M, rows)
        table[1, :, :M] = np.sin(angle).reshape(Y_BLOCKS, M, rows)
        tables.append(stacked(table.reshape(2 * Y_BLOCKS * MP, rows)))
    return np.stack(tables)


def x_table():
    angle = angles(kept(NX, MX), np.arange(NX), NX).T
    table = np.zeros((NX, 2, LANES))
    table[:, 0, :MX] = np.cos(angle)
    table[:, 1, :MX] = np.sin(angle)
    return halves(table.reshape(NX, 2 * LANES))


def y_inverse_table(y_devices):
    tables = []
    rows = NY // y_devices
    for d in range(y_devices):
        angle = angles(kept(NY, MY), d * rows + np.arange(rows), NY).T
        table = np.zeros((2, rows, 2, Y_BLOCKS, MP))
        cosine = np.cos(angle).reshape(rows, Y_BLOCKS, M)
        sine = np.sin(angle).reshape(rows, Y_BLOCKS, M)
        table[0, :, 0, :, :M] = cosine
        table[0, :, 1, :, :M] = -sine
        table[1, :, 0, :, :M] = sine
        table[1, :, 1, :, :M] = cosine
        tables.append(stacked(table.reshape(2 * rows, 2 * Y_BLOCKS * MP)))
    return np.stack(tables)


def z_inverse_table(y_devices):
    tables = []
    for kz in z_order(y_devices):
        angle = angles(kz, np.arange(NZ), NZ)
        weight = np.where(kz == 0, 1.0, 2.0)[:, None] / (NX * NY * NZ)
        cosine = np.tile(np.cos(angle) * weight, (QUAD, 1))
        sine = np.tile(np.sin(angle) * weight, (QUAD, 1))
        tables.append(halves(np.concatenate([cosine, -sine], 0)))
    return np.stack(tables)


def own_block(table, c, dim):
    at = lax.broadcasted_iota(jnp.int32, table.shape, dim) // MZ % QUAD
    return jnp.where(at == c, table.astype(jnp.float32), 0.0).astype(jnp.bfloat16)


def forward_kernel(place, field, z_table, y_table, own, other, spread, z_hat, rows):
    del place
    first_x = pl.program_id(0) * X_STEP

    @pl.when(pl.program_id(0) == 0)
    def _():
        for part in range(2):
            for c in range(QUAD):
                spread[part, c * NZ : (c + 1) * NZ, :] = own_block(z_table[0, part], c, 1)

    channels, _, y_local, _ = field.shape
    groups = channels // QUAD
    per_x = QUAD * MZ
    half = MZ // 2
    size = Y_BLOCKS * MP
    stride = Y_BLOCKS * own.shape[1]
    cells = jnp.concatenate(
        [
            jnp.concatenate([field[QUAD * g + c, i] for c in range(QUAD)], 1)
            for i in range(X_STEP)
            for g in range(groups)
        ],
        0,
    )
    z_hat[...] = dot(cells, spread[0]) + dot(cells, spread[1])
    own_rows = own.reshape(own.shape[0] * own.shape[1], LANES)
    other_rows = other.reshape(other.shape[0] * other.shape[1], LANES)
    for i in range(X_STEP):
        for g in range(groups):
            high, low = split(z_hat[pl.ds((i * groups + g) * y_local, y_local), :])
            parts = dot(y_table[0], jnp.concatenate([high, low], 0))
            parts = parts[: 2 * size] + parts[2 * size :]
            real = parts[:size, :per_x] + parts[size:, per_x:]
            imag = parts[:size, per_x:] - parts[size:, :per_x]
            for block in range(Y_BLOCKS):
                for s, value in enumerate((real, imag)):
                    at = pl.ds(s * HALF + g * M, MP)
                    rows[i, block, at, :] = value[block * MP : (block + 1) * MP]
        for block in range(Y_BLOCKS):
            turned = rows[i, block, :LANES, :].T
            for c in range(QUAD):
                start = block * own.shape[1] + (first_x + i) * QUAD + c
                at = pl.ds(start, half, stride=stride)
                own_rows[at, :] = turned[c * MZ : c * MZ + half]
                other_rows[at, :] = turned[c * MZ + half : (c + 1) * MZ]


def forward(place, field, y_devices, x_devices):
    channels, x_local, y_local, _ = field.shape
    z_table, y_table = z_forward_table(y_devices), y_forward_table(y_devices)
    payload = jax.ShapeDtypeStruct((x_devices, x_local * QUAD, LANES), jnp.float32)
    whole = pl.BlockSpec(payload.shape, lambda x, p: (0, 0, 0))
    lines = X_STEP * (channels // QUAD) * y_local
    return pl.pallas_call(
        forward_kernel,
        out_shape=(payload, payload),
        grid_spec=pltpu.PrefetchScalarGridSpec(
            num_scalar_prefetch=1,
            grid=(x_local // X_STEP,),
            in_specs=[
                pl.BlockSpec((channels, X_STEP, y_local, NZ), lambda x, p: (0, x, 0, 0)),
                pl.BlockSpec((1, *z_table.shape[1:]), lambda x, p: (p[0], 0, 0, 0)),
                pl.BlockSpec((1, *y_table.shape[1:]), lambda x, p: (p[0], 0, 0)),
            ],
            out_specs=[whole, whole],
            scratch_shapes=[
                pltpu.VMEM((2, QUAD * NZ, 2 * QUAD * MZ), jnp.bfloat16),
                pltpu.VMEM((lines, 2 * QUAD * MZ), jnp.float32),
                pltpu.VMEM((X_STEP, Y_BLOCKS, LANES + MP, LANES), jnp.float32),
            ],
        ),
        compiler_params=pltpu.CompilerParams(
            dimension_semantics=("arbitrary",), vmem_limit_bytes=20 * MIB
        ),
        name="forward",
    )(place, field, jnp.asarray(z_table), jnp.asarray(y_table))


def mix_kernel(payload, weights, table, result, spectrum, mixed):
    channels = weights.shape[1]
    source = payload.reshape(payload.shape[0] * payload.shape[1], LANES)
    target = result.reshape(result.shape[0] * result.shape[1], LANES)
    rows = jnp.concatenate([source[pl.ds(c, NX, stride=QUAD), :] for c in range(QUAD)], 1)
    high, low = split(rows.T)
    parts = dot(high, table[0]) + dot(low, table[0]) + dot(high, table[1])
    for c in range(QUAD):
        upper = parts[c * LANES : c * LANES + HALF]
        lower = parts[c * LANES + HALF : (c + 1) * LANES]
        spectrum[c, 0] = upper[:, :LANES] + lower[:, LANES:]
        spectrum[c, 1] = lower[:, :LANES] - upper[:, LANES:]
    outs = channels // 2
    for first in range(0, channels, outs):
        real = [jnp.zeros((MP, LANES), jnp.float32)] * outs
        imag = [jnp.zeros((MP, LANES), jnp.float32)] * outs
        for i in range(channels):
            g, c = i // QUAD, i % QUAD
            real_in = spectrum[c, 0, pl.ds(g * M, MP), :]
            imag_in = spectrum[c, 1, pl.ds(g * M, MP), :]
            for k in range(outs):
                w_real = weights[0, i, first + k].astype(jnp.float32)
                w_imag = weights[1, i, first + k].astype(jnp.float32)
                real[k] = real[k] + (w_real * real_in - w_imag * imag_in)
                imag[k] = imag[k] + (w_real * imag_in + w_imag * real_in)
        for k in range(outs):
            g, c = (first + k) // QUAD, (first + k) % QUAD
            upper = pl.ds(g * M, MP)
            lower = pl.ds(HALF + g * M, MP)
            mixed[c, upper, :LANES] = real[k]
            mixed[c, upper, LANES:] = -imag[k]
            mixed[c, lower, :LANES] = imag[k]
            mixed[c, lower, LANES:] = real[k]
    for c in range(0, QUAD, 2):
        high, low = split(jnp.concatenate([mixed[c, :LANES, :], mixed[c + 1, :LANES, :]], 0))
        over_k = ((1,), (1,))
        back = dot(table[0], high, over_k) + dot(table[0], low, over_k) + dot(table[1], high, over_k)
        target[pl.ds(c, NX, stride=QUAD), :] = back[:, :LANES]
        target[pl.ds(c + 1, NX, stride=QUAD), :] = back[:, LANES:]


def mix(payload, weights):
    table = x_table()
    vmem = pl.BlockSpec(memory_space=pltpu.VMEM)
    return pl.pallas_call(
        mix_kernel,
        out_shape=jax.ShapeDtypeStruct(payload.shape, jnp.float32),
        in_specs=[vmem, vmem, vmem],
        out_specs=vmem,
        scratch_shapes=[
            pltpu.VMEM((QUAD, 2, HALF, LANES), jnp.float32),
            pltpu.VMEM((QUAD, LANES + MP, 2 * LANES), jnp.float32),
        ],
        compiler_params=pltpu.CompilerParams(vmem_limit_bytes=20 * MIB),
        name="mix",
    )(payload, weights, jnp.asarray(table))


def pointwise_kernel(field, local, bias, out):
    channels, steps, y_local, _ = field.shape
    for i in range(steps):
        for y in range(0, y_local, 2 * MP):
            pair = [
                field[:, i, y + j * MP : y + (j + 1) * MP, :].reshape(channels * MP, NZ) for j in range(2)
            ]
            mixed = dot(local[...], jnp.concatenate(pair, 1))
            for o in range(channels):
                for j in range(2):
                    value = mixed[o * MP : (o + 1) * MP, j * NZ : (j + 1) * NZ]
                    out[o, i, y + j * MP : y + (j + 1) * MP, :] = value + bias[o]


def pointwise(field, local, bias):
    channels, x_local, y_local, _ = field.shape
    cells = pl.BlockSpec((channels, 1, y_local, NZ), lambda x: (0, x, 0, 0))
    return pl.pallas_call(
        pointwise_kernel,
        out_shape=jax.ShapeDtypeStruct(field.shape, jnp.float32),
        grid=(x_local,),
        in_specs=[cells, pl.BlockSpec(local.shape, lambda x: (0, 0)), pl.BlockSpec(memory_space=pltpu.SMEM)],
        out_specs=cells,
        compiler_params=pltpu.CompilerParams(
            dimension_semantics=("arbitrary",), vmem_limit_bytes=12 * MIB
        ),
        cost_estimate=pl.CostEstimate(
            flops=2 * field.size * channels * MP, transcendentals=0, bytes_accessed=6 * field.size
        ),
        name="pointwise",
    )(field, local, bias)


def inverse_kernel(place, own, other, base, y_table, z_table, out, spread, rows, modes, lines, total):
    del place
    first_x = pl.program_id(0) * X_STEP

    @pl.when(pl.program_id(0) == 0)
    def _():
        for part in range(2):
            for c in range(QUAD):
                spread[part, :, c * NZ : (c + 1) * NZ] = own_block(z_table[0, part], c, 0)

    channels, _, y_local, _ = base.shape
    groups = channels // QUAD
    half = MZ // 2
    stride = Y_BLOCKS * own.shape[1]
    own_rows = own.reshape(own.shape[0] * own.shape[1], LANES)
    other_rows = other.reshape(other.shape[0] * other.shape[1], LANES)
    for i in range(X_STEP):
        for block in range(Y_BLOCKS):
            for c in range(QUAD):
                start = block * own.shape[1] + (first_x + i) * QUAD + c
                at = pl.ds(start, half, stride=stride)
                rows[i, block, c * MZ : c * MZ + half] = own_rows[at, :]
                rows[i, block, c * MZ + half : (c + 1) * MZ] = other_rows[at, :]
            modes[i, block] = rows[i, block].T
    for g in range(groups):
        inputs = jnp.concatenate(
            [
                jnp.concatenate([modes[i, block, pl.ds(s * HALF + g * M, MP), :] for i in range(X_STEP)], 1)
                for s in range(2)
                for block in range(Y_BLOCKS)
            ],
            0,
        )
        high, low = split(inputs)
        parts = dot(y_table[0], jnp.concatenate([high, low], 0))
        parts = parts[: 2 * y_local] + parts[2 * y_local :]
        for i in range(X_STEP):
            at = pl.ds((i * groups + g) * y_local, y_local)
            for s in range(2):
                high, low = split(parts[s * y_local : (s + 1) * y_local, i * LANES : (i + 1) * LANES])
                lines[0, at, s * LANES : (s + 1) * LANES] = high
                lines[1, at, s * LANES : (s + 1) * LANES] = low
    total[...] = dot(lines[0], spread[0]) + dot(lines[1], spread[0]) + dot(lines[0], spread[1])
    first = math.sqrt(2 / math.pi)
    for i in range(X_STEP):
        for o in range(channels):
            g, c = o // QUAD, o % QUAD
            at = pl.ds((i * groups + g) * y_local, y_local)
            value = total[at, c * NZ : (c + 1) * NZ] + base[o, i]
            inner = value * (first + (first * 0.044715) * (value * value))
            scaled = 0.5 * value
            out[o, i] = (scaled + scaled * jnp.tanh(inner)).astype(out.dtype)


def inverse(place, own, other, base, y_devices, dtype):
    channels, x_local, y_local, _ = base.shape
    z_table, y_table = z_inverse_table(y_devices), y_inverse_table(y_devices)
    whole = pl.BlockSpec(own.shape, lambda x, p: (0, 0, 0))
    cells = pl.BlockSpec((channels, X_STEP, y_local, NZ), lambda x, p: (0, x, 0, 0))
    lines = X_STEP * (channels // QUAD) * y_local
    return pl.pallas_call(
        inverse_kernel,
        out_shape=jax.ShapeDtypeStruct(base.shape, dtype),
        grid_spec=pltpu.PrefetchScalarGridSpec(
            num_scalar_prefetch=1,
            grid=(x_local // X_STEP,),
            in_specs=[
                whole,
                whole,
                cells,
                pl.BlockSpec((1, *y_table.shape[1:]), lambda x, p: (p[0], 0, 0)),
                pl.BlockSpec((1, *z_table.shape[1:]), lambda x, p: (p[0], 0, 0, 0)),
            ],
            out_specs=cells,
            scratch_shapes=[
                pltpu.VMEM((2, 2 * QUAD * MZ, QUAD * NZ), jnp.bfloat16),
                pltpu.VMEM((X_STEP, Y_BLOCKS, LANES, LANES), jnp.float32),
                pltpu.VMEM((X_STEP, Y_BLOCKS, LANES, LANES), jnp.float32),
                pltpu.VMEM((2, lines, 2 * LANES), jnp.bfloat16),
                pltpu.VMEM((lines, QUAD * NZ), jnp.float32),
            ],
        ),
        compiler_params=pltpu.CompilerParams(
            dimension_semantics=("arbitrary",), vmem_limit_bytes=28 * MIB
        ),
        name="inverse",
    )(place, own, other, base, jnp.asarray(y_table), jnp.asarray(z_table))


def spread_weights(spectral_weight):
    m, k = spectral_weight.shape[3:]
    return jnp.pad(spectral_weight, ((0, 0), (0, 0), (0, 0), (0, MP - m), (0, LANES - k)))


def local_matrix(pointwise_weight):
    channels = pointwise_weight.shape[0]
    eye = jnp.eye(MP, dtype=pointwise_weight.dtype)
    matrix = pointwise_weight.T[:, None, :, None] * eye[None, :, None, :]
    return matrix.reshape(channels * MP, channels * MP)


def swapped(x, axis):
    devices = lax.axis_size(axis)
    return lax.ppermute(x, axis, [(d, (d + 1) % devices) for d in range(devices)])


def per_device(field, spectral_weight, pointwise_weight, bias):
    y_devices, x_devices = lax.axis_size("py"), lax.axis_size("px")
    place = lax.axis_index("py").astype(jnp.int32).reshape(1)
    cells = field[0]
    own, other = forward(place, cells, y_devices, x_devices)
    payload = own + swapped(other, "py")
    payload, spectral_weight, pointwise_weight, bias = lax.optimization_barrier(
        (payload, spectral_weight, pointwise_weight, bias)
    )
    received = lax.all_to_all(payload, "px", 0, 0, tiled=True)
    weights = spread_weights(spectral_weight)
    base = pointwise(cells, local_matrix(pointwise_weight), bias)
    received, base = lax.optimization_barrier((received, base))
    result = mix(received, weights)
    own = lax.all_to_all(result, "px", 0, 0, tiled=True)
    other = swapped(own, "py")
    return inverse(place, own, other, base, y_devices, field.dtype)[None]


def solution(mesh):
    in_specs = (
        P("groups", None, "px", "py", None),
        P(None, None, None, ("py", "px"), None),
        P(),
        P(),
    )
    out_specs = P("groups", None, "px", "py", None)
    return jax.shard_map(per_device, mesh=mesh, in_specs=in_specs, out_specs=out_specs, check_vma=False)
```

```python
import functools
import math

import jax
import jax.numpy as jnp
import numpy as np
from jax import lax
from jax.experimental import pallas as pl
from jax.experimental.pallas import tpu as pltpu
from jax.sharding import PartitionSpec as P

NX = 384
NY = 192
NZ = 128
MX = 96
MY = 48
MZ = 32

LANES = 128
QUAD = 4
Y_BLOCKS = 4
M = MY // Y_BLOCKS
MP = 16
HALF = 64
SPARE = 4
X_FORWARD = 3
X_INVERSE = 2
MIB = 1024 * 1024


def kept(length, retained):
    index = np.arange(retained)
    return np.where(index < retained // 2, index, length - retained + index)


def angles(frequency, positions, length):
    return 2 * np.pi * ((frequency[:, None] * positions[None, :]) % length) / length


def halves(table):
    high = table.astype(np.float32).astype(jnp.bfloat16)
    low = (table - high.astype(np.float64)).astype(np.float32).astype(jnp.bfloat16)
    return np.stack([high, low])


def split(value):
    high = value.astype(jnp.bfloat16)
    low = (value - high.astype(jnp.float32)).astype(jnp.bfloat16)
    return high, low


def in_hbm(array):
    return pltpu.with_memory_space_constraint(array, pltpu.HBM)


def dot(a, b, contract=((1,), (0,))):
    return lax.dot_general(a, b, (contract, ((), ())), preferred_element_type=jnp.float32)


def z_order(y_devices):
    order = np.arange(MZ).reshape(y_devices, MZ // y_devices)
    return [np.concatenate([order[d], np.delete(order, d, 0).reshape(-1)]) for d in range(y_devices)]


def z_forward_table(y_devices):
    tables = []
    for kz in z_order(y_devices):
        angle = np.tile(angles(kz, np.arange(NZ), NZ).T, (1, QUAD))
        tables.append(halves(np.concatenate([np.cos(angle), -np.sin(angle)], 1)))
    return np.stack(tables)


def stacked(table):
    high, low = halves(table)
    return np.concatenate([np.concatenate([high, high], 1), np.concatenate([low, np.zeros_like(low)], 1)], 0)


def y_forward_table(y_devices):
    tables = []
    rows = NY // y_devices
    for d in range(y_devices):
        angle = angles(kept(NY, MY), d * rows + np.arange(rows), NY)
        table = np.zeros((2, Y_BLOCKS, MP, rows))
        table[0, :, :M] = np.cos(angle).reshape(Y_BLOCKS, M, rows)
        table[1, :, :M] = np.sin(angle).reshape(Y_BLOCKS, M, rows)
        tables.append(stacked(table.reshape(2 * Y_BLOCKS * MP, rows)))
    return np.stack(tables)


def x_table(x_local):
    angle = angles(kept(NX, MX), np.arange(NX).reshape(-1, x_local).T.reshape(-1), NX).T
    table = np.zeros((NX, 2, LANES))
    table[:, 0, :MX] = np.cos(angle)
    table[:, 1, :MX] = np.sin(angle)
    return halves(table.reshape(NX, 2 * LANES))


def y_inverse_table(y_devices):
    tables = []
    rows = NY // y_devices
    for d in range(y_devices):
        angle = angles(kept(NY, MY), d * rows + np.arange(rows), NY).T
        table = np.zeros((2, rows, 2, Y_BLOCKS, MP))
        cosine = np.cos(angle).reshape(rows, Y_BLOCKS, M)
        sine = np.sin(angle).reshape(rows, Y_BLOCKS, M)
        table[0, :, 0, :, :M] = cosine
        table[0, :, 1, :, :M] = -sine
        table[1, :, 0, :, :M] = sine
        table[1, :, 1, :, :M] = cosine
        tables.append(stacked(table.reshape(2 * rows, 2 * Y_BLOCKS * MP)))
    return np.stack(tables)


def z_inverse_table(y_devices):
    tables = []
    for kz in z_order(y_devices):
        angle = angles(kz, np.arange(NZ), NZ)
        weight = np.where(kz == 0, 1.0, 2.0)[:, None] / (NX * NY * NZ)
        cosine = np.tile(np.cos(angle) * weight, (QUAD, 1))
        sine = np.tile(np.sin(angle) * weight, (QUAD, 1))
        tables.append(halves(np.concatenate([cosine, -sine], 0)))
    return np.stack(tables)


def own_block(table, c, dim):
    at = lax.broadcasted_iota(jnp.int32, table.shape, dim) // MZ % QUAD
    return jnp.where(at == c, table.astype(jnp.float32), 0.0).astype(jnp.bfloat16)


def lane_of_part(shape):
    return lax.broadcasted_iota(jnp.int32, shape, len(shape) - 1) % HALF


def with_spare(row, value, last):
    used = HALF - SPARE
    if row >= used // SPARE:
        return value
    moved = pltpu.roll(last, used - SPARE * row, 1)
    return jnp.where(lane_of_part(value.shape) >= used, moved, value)


def last_row(value_of_row):
    used = HALF - SPARE
    result = value_of_row(0)
    at = lane_of_part(result.shape) // SPARE
    result = pltpu.roll(result, LANES - used, 1)
    for row in range(1, used // SPARE):
        moved = pltpu.roll(value_of_row(row), LANES - used + SPARE * row, 1)
        result = jnp.where(at == row, moved, result)
    return result


def forward_kernel(
    x_local, place, field, z_tables, y_tables, own, other, cells, z_table, y_table, spread, z_hat, rows, loaded
):
    channels, _, y_local, _ = field.shape
    groups = channels // QUAD
    per_x = QUAD * MZ
    half = MZ // 2
    size = Y_BLOCKS * MP
    sent = x_local * QUAD - 1
    order = list(range(x_local))[::-1]
    loads = [pltpu.make_async_copy(field.at[:, x], cells.at[x], loaded.at[x]) for x in range(x_local)]
    tables = [
        pltpu.make_async_copy(z_tables.at[place[0]], z_table, loaded.at[x_local]),
        pltpu.make_async_copy(y_tables.at[place[0]], y_table, loaded.at[x_local + 1]),
    ]
    tables[0].start()
    for x in order[:X_FORWARD]:
        loads[x].start()
    tables[1].start()
    for x in order[X_FORWARD:]:
        loads[x].start()
    tables[0].wait()
    for part in range(2):
        for c in range(QUAD):
            spread[part, c * NZ : (c + 1) * NZ, :] = own_block(z_table[part], c, 1)
    last = {}
    for first in range(0, x_local, X_FORWARD):
        chunk = order[first : first + X_FORWARD]
        for x in chunk:
            loads[x].wait()
        inputs = jnp.concatenate(
            [
                jnp.concatenate([cells[x, QUAD * g + c] for c in range(QUAD)], 1)
                for x in chunk
                for g in range(groups)
            ],
            0,
        )
        z_hat[first // X_FORWARD] = dot(inputs, spread[0]) + dot(inputs, spread[1])
        if first == 0:
            tables[1].wait()
        for i, x in enumerate(chunk):
            for g in range(groups):
                at = pl.ds((i * groups + g) * y_local, y_local)
                high, low = split(z_hat[first // X_FORWARD, at, :])
                parts = dot(y_table[...], jnp.concatenate([high, low], 0))
                parts = parts[: 2 * size] + parts[2 * size :]
                real = parts[:size, :per_x] + parts[size:, per_x:]
                imag = parts[:size, per_x:] - parts[size:, :per_x]
                for block in range(Y_BLOCKS):
                    for s, value in enumerate((real, imag)):
                        at = pl.ds(s * HALF + g * M, MP)
                        rows[x, block, at, :] = value[block * MP : (block + 1) * MP]
            for block in range(Y_BLOCKS):
                turned = rows[x, block, :LANES, :].T
                for c in reversed(range(QUAD)):
                    row = x * QUAD + c
                    for k, out in enumerate((own, other)):
                        value = turned[c * MZ + k * half : c * MZ + (k + 1) * half]
                        if row == sent:
                            last[block, k] = value
                        else:
                            at = pl.ds(block * sent + row, half, stride=Y_BLOCKS * sent)
                            out[at, :] = with_spare(row, value, last[block, k])


def forward(place, field, y_devices, x_devices):
    channels, x_local, y_local, _ = field.shape
    z_table, y_table = z_forward_table(y_devices), y_forward_table(y_devices)
    payload = jax.ShapeDtypeStruct((x_devices * (x_local * QUAD - 1), LANES), jnp.float32)
    lines = X_FORWARD * (channels // QUAD) * y_local
    vmem = pl.BlockSpec(memory_space=pltpu.VMEM)
    return pl.pallas_call(
        functools.partial(forward_kernel, x_local),
        out_shape=(payload, payload),
        grid_spec=pltpu.PrefetchScalarGridSpec(
            num_scalar_prefetch=1,
            grid=(1,),
            in_specs=[pl.BlockSpec(memory_space=pltpu.HBM)] * 3,
            out_specs=[vmem, vmem],
            scratch_shapes=[
                pltpu.VMEM((x_local, channels, y_local, NZ), field.dtype),
                pltpu.VMEM(z_table.shape[1:], jnp.bfloat16),
                pltpu.VMEM(y_table.shape[1:], jnp.bfloat16),
                pltpu.VMEM((2, QUAD * NZ, 2 * QUAD * MZ), jnp.bfloat16),
                pltpu.VMEM((x_local // X_FORWARD, lines, 2 * QUAD * MZ), jnp.float32),
                pltpu.VMEM((x_local, Y_BLOCKS, LANES + MP, LANES), jnp.float32),
                pltpu.SemaphoreType.DMA((x_local + 2,)),
            ],
        ),
        compiler_params=pltpu.CompilerParams(
            dimension_semantics=("arbitrary",), vmem_limit_bytes=24 * MIB
        ),
        name="forward",
    )(place, in_hbm(field), in_hbm(jnp.asarray(z_table)), in_hbm(jnp.asarray(y_table)))


def mix_kernel(x_local, payload, weights, table_hbm, result, table, spectrum, mixed, done):
    channels = weights.shape[1]
    sent = x_local * QUAD - 1
    x_devices = payload.shape[0] // sent
    load = pltpu.make_async_copy(table_hbm, table, done)
    load.start()

    def row_of(row):
        return pl.ds(row, x_devices, stride=sent)

    lines = [payload[row_of(row), :] for row in range(sent)]
    lines.append(last_row(lambda row: lines[row]))
    rows = jnp.concatenate([jnp.concatenate(lines[c::QUAD], 0) for c in range(QUAD)], 1)
    high, low = split(rows.T)
    load.wait()
    parts = dot(high, table[0]) + dot(low, table[0]) + dot(high, table[1])
    for c in range(QUAD):
        upper = parts[c * LANES : c * LANES + HALF]
        lower = parts[c * LANES + HALF : (c + 1) * LANES]
        spectrum[c, 0] = upper[:, :LANES] + lower[:, LANES:]
        spectrum[c, 1] = lower[:, :LANES] - upper[:, LANES:]
    outs = channels // 2
    for first in range(0, channels, outs):
        real = [jnp.zeros((MP, LANES), jnp.float32)] * outs
        imag = [jnp.zeros((MP, LANES), jnp.float32)] * outs
        for i in range(channels):
            g, c = i // QUAD, i % QUAD
            real_in = spectrum[c, 0, pl.ds(g * M, MP), :]
            imag_in = spectrum[c, 1, pl.ds(g * M, MP), :]
            for k in range(outs):
                w_real = weights[0, i, first + k].astype(jnp.float32)
                w_imag = weights[1, i, first + k].astype(jnp.float32)
                real[k] = real[k] + (w_real * real_in - w_imag * imag_in)
                imag[k] = imag[k] + (w_real * imag_in + w_imag * real_in)
        for k in range(outs):
            g, c = (first + k) // QUAD, (first + k) % QUAD
            upper = pl.ds(g * M, MP)
            lower = pl.ds(HALF + g * M, MP)
            mixed[c, upper, :LANES] = real[k]
            mixed[c, upper, LANES:] = -imag[k]
            mixed[c, lower, :LANES] = imag[k]
            mixed[c, lower, LANES:] = real[k]
    last = None
    for c in range(QUAD - 2, -1, -2):
        high, low = split(jnp.concatenate([mixed[c, :LANES, :], mixed[c + 1, :LANES, :]], 0))
        over_k = ((1,), (1,))
        back = dot(table[0], high, over_k) + dot(table[0], low, over_k) + dot(table[1], high, over_k)
        if last is None:
            last = back[(x_local - 1) * x_devices :, LANES:]
        for x in range(x_local):
            for k in range(2):
                row = x * QUAD + c + k
                if row < sent:
                    value = back[x * x_devices : (x + 1) * x_devices, k * LANES : (k + 1) * LANES]
                    result[row_of(row), :] = with_spare(row, value, last)


def mix(payload, weights, x_local):
    table = x_table(x_local)
    vmem = pl.BlockSpec(memory_space=pltpu.VMEM)
    return pl.pallas_call(
        functools.partial(mix_kernel, x_local),
        out_shape=jax.ShapeDtypeStruct(payload.shape, jnp.float32),
        in_specs=[vmem, vmem, pl.BlockSpec(memory_space=pltpu.HBM)],
        out_specs=vmem,
        scratch_shapes=[
            pltpu.VMEM(table.shape, jnp.bfloat16),
            pltpu.VMEM((QUAD, 2, HALF, LANES), jnp.float32),
            pltpu.VMEM((QUAD, LANES + MP, 2 * LANES), jnp.float32),
            pltpu.SemaphoreType.DMA,
        ],
        compiler_params=pltpu.CompilerParams(vmem_limit_bytes=20 * MIB),
        name="mix",
    )(payload, weights, in_hbm(jnp.asarray(table)))


def pointwise_kernel(field, local, bias, out):
    channels, steps, y_local, _ = field.shape
    for i in range(steps):
        for y in range(0, y_local, 2 * MP):
            pair = [
                field[:, i, y + j * MP : y + (j + 1) * MP, :].reshape(channels * MP, NZ) for j in range(2)
            ]
            mixed = dot(local[...], jnp.concatenate(pair, 1))
            for o in range(channels):
                for j in range(2):
                    value = mixed[o * MP : (o + 1) * MP, j * NZ : (j + 1) * NZ]
                    out[o, i, y + j * MP : y + (j + 1) * MP, :] = value + bias[o]


def pointwise(field, local, bias):
    channels, x_local, y_local, _ = field.shape
    cells = pl.BlockSpec((channels, 1, y_local, NZ), lambda x: (0, x, 0, 0))
    return pl.pallas_call(
        pointwise_kernel,
        out_shape=jax.ShapeDtypeStruct(field.shape, jnp.float32),
        grid=(x_local,),
        in_specs=[cells, pl.BlockSpec(local.shape, lambda x: (0, 0)), pl.BlockSpec(memory_space=pltpu.SMEM)],
        out_specs=cells,
        compiler_params=pltpu.CompilerParams(
            dimension_semantics=("arbitrary",), vmem_limit_bytes=12 * MIB
        ),
        cost_estimate=pl.CostEstimate(
            flops=2 * field.size * channels * MP, transcendentals=0, bytes_accessed=6 * field.size
        ),
        name="pointwise",
    )(field, local, bias)


def inverse_kernel(place, own, other, base, y_table, z_table, out, spread, rows, modes, lines, total, cells, stored):
    del place
    channels, x_local, y_local, _ = base.shape
    groups = channels // QUAD
    half = MZ // 2
    sent = x_local * QUAD - 1
    for part in range(2):
        for c in range(QUAD):
            spread[part, :, c * NZ : (c + 1) * NZ] = own_block(z_table[0, part], c, 0)

    def row_of(block, row):
        return pl.ds(block * sent + row, half, stride=Y_BLOCKS * sent)

    stores = [pltpu.make_async_copy(cells.at[x], out.at[:, x], stored.at[x]) for x in range(x_local)]
    for first in range(0, x_local, X_INVERSE):
        chunk = range(first, first + X_INVERSE)
        for x in chunk:
            for block in range(Y_BLOCKS):
                for c in range(QUAD):
                    for k, source in enumerate((own, other)):
                        row = x * QUAD + c
                        if row < sent:
                            value = source[row_of(block, row), :]
                        else:
                            value = last_row(lambda r: source[row_of(block, r), :])
                        rows[x, block, c * MZ + k * half : c * MZ + (k + 1) * half] = value
                modes[x, block] = rows[x, block].T
        for g in range(groups):
            inputs = jnp.concatenate(
                [
                    jnp.concatenate([modes[x, block, pl.ds(s * HALF + g * M, MP), :] for x in chunk], 1)
                    for s in range(2)
                    for block in range(Y_BLOCKS)
                ],
                0,
            )
            high, low = split(inputs)
            parts = dot(y_table[0], jnp.concatenate([high, low], 0))
            parts = parts[: 2 * y_local] + parts[2 * y_local :]
            for i in range(X_INVERSE):
                at = pl.ds(((first + i) * groups + g) * y_local, y_local)
                for s in range(2):
                    high, low = split(parts[s * y_local : (s + 1) * y_local, i * LANES : (i + 1) * LANES])
                    lines[0, at, s * LANES : (s + 1) * LANES] = high
                    lines[1, at, s * LANES : (s + 1) * LANES] = low
        at = pl.ds(first * groups * y_local, X_INVERSE * groups * y_local)
        high, low = lines[0, at, :], lines[1, at, :]
        total[at, :] = dot(high, spread[0]) + dot(low, spread[0]) + dot(high, spread[1])
        scale = math.sqrt(2 / math.pi)
        for x in chunk:
            for o in range(channels):
                g, c = o // QUAD, o % QUAD
                at = pl.ds((x * groups + g) * y_local, y_local)
                value = total[at, c * NZ : (c + 1) * NZ] + base[o, x]
                inner = value * (scale + (scale * 0.044715) * (value * value))
                scaled = 0.5 * value
                cells[x, o] = (scaled + scaled * jnp.tanh(inner)).astype(out.dtype)
            stores[x].start()
    for store in stores:
        store.wait()


def inverse(place, own, other, base, y_devices, dtype):
    channels, x_local, y_local, _ = base.shape
    z_table, y_table = z_inverse_table(y_devices), y_inverse_table(y_devices)
    vmem = pl.BlockSpec(memory_space=pltpu.VMEM)
    lines = x_local * (channels // QUAD) * y_local
    return pl.pallas_call(
        inverse_kernel,
        out_shape=jax.ShapeDtypeStruct(base.shape, dtype),
        grid_spec=pltpu.PrefetchScalarGridSpec(
            num_scalar_prefetch=1,
            grid=(1,),
            in_specs=[
                vmem,
                vmem,
                vmem,
                pl.BlockSpec((1, *y_table.shape[1:]), lambda x, p: (p[0], 0, 0)),
                pl.BlockSpec((1, *z_table.shape[1:]), lambda x, p: (p[0], 0, 0, 0)),
            ],
            out_specs=pl.BlockSpec(memory_space=pltpu.HBM),
            scratch_shapes=[
                pltpu.VMEM((2, 2 * QUAD * MZ, QUAD * NZ), jnp.bfloat16),
                pltpu.VMEM((x_local, Y_BLOCKS, LANES, LANES), jnp.float32),
                pltpu.VMEM((x_local, Y_BLOCKS, LANES, LANES), jnp.float32),
                pltpu.VMEM((2, lines, 2 * LANES), jnp.bfloat16),
                pltpu.VMEM((lines, QUAD * NZ), jnp.float32),
                pltpu.VMEM((x_local, channels, y_local, NZ), dtype),
                pltpu.SemaphoreType.DMA((x_local,)),
            ],
        ),
        compiler_params=pltpu.CompilerParams(
            dimension_semantics=("arbitrary",), vmem_limit_bytes=36 * MIB
        ),
        name="inverse",
    )(place, own, other, base, jnp.asarray(y_table), jnp.asarray(z_table))


def spread_weights(spectral_weight):
    m, k = spectral_weight.shape[3:]
    return jnp.pad(spectral_weight, ((0, 0), (0, 0), (0, 0), (0, MP - m), (0, LANES - k)))


def local_matrix(pointwise_weight):
    channels = pointwise_weight.shape[0]
    eye = jnp.eye(MP, dtype=pointwise_weight.dtype)
    matrix = pointwise_weight.T[:, None, :, None] * eye[None, :, None, :]
    return matrix.reshape(channels * MP, channels * MP)


def swapped(x, axis):
    devices = lax.axis_size(axis)
    return lax.ppermute(x, axis, [(d, (d + 1) % devices) for d in range(devices)])


def exchanged(rows, axis):
    devices = lax.axis_size(axis)
    blocks = rows.reshape(devices, rows.shape[0] // devices, 1, LANES)
    return lax.all_to_all(blocks, axis, 0, 0, tiled=True).reshape(rows.shape)


def per_device(field, spectral_weight, pointwise_weight, bias):
    y_devices, x_devices = lax.axis_size("py"), lax.axis_size("px")
    place = lax.axis_index("py").astype(jnp.int32).reshape(1)
    cells = field[0]
    own, other = forward(place, cells, y_devices, x_devices)
    payload = own + swapped(other, "py")
    payload, spectral_weight, pointwise_weight, bias = lax.optimization_barrier(
        (payload, spectral_weight, pointwise_weight, bias)
    )
    received = exchanged(payload, "px")
    weights = spread_weights(spectral_weight)
    base = pointwise(cells, local_matrix(pointwise_weight), bias)
    received, base = lax.optimization_barrier((received, base))
    result = mix(received, weights, cells.shape[1])
    own = exchanged(result, "px")
    other = swapped(own, "py")
    return inverse(place, own, other, base, y_devices, field.dtype)[None]


def solution(mesh):
    in_specs = (
        P("groups", None, "px", "py", None),
        P(None, None, None, ("py", "px"), None),
        P(),
        P(),
    )
    out_specs = P("groups", None, "px", "py", None)
    return jax.shard_map(per_device, mesh=mesh, in_specs=in_specs, out_specs=out_specs, check_vma=False)
```

```python
import functools
import math

import jax
import jax.numpy as jnp
import numpy as np
from jax import lax
from jax.experimental import pallas as pl
from jax.experimental.pallas import tpu as pltpu
from jax.sharding import PartitionSpec as P

NX = 384
NY = 192
NZ = 128
MX = 96
MY = 48
MZ = 32

LANES = 128
QUAD = 4
Y_BLOCKS = 4
M = MY // Y_BLOCKS
MP = 16
HALF = 64
SPARE = 4
X_FORWARD = 3
X_INVERSE = 2
MIB = 1024 * 1024


def kept(length, retained):
    index = np.arange(retained)
    return np.where(index < retained // 2, index, length - retained + index)


def angles(frequency, positions, length):
    return 2 * np.pi * ((frequency[:, None] * positions[None, :]) % length) / length


def halves(table):
    high = table.astype(np.float32).astype(jnp.bfloat16)
    low = (table - high.astype(np.float64)).astype(np.float32).astype(jnp.bfloat16)
    return np.stack([high, low])


def split(value):
    high = value.astype(jnp.bfloat16)
    low = (value - high.astype(jnp.float32)).astype(jnp.bfloat16)
    return high, low


def in_hbm(array):
    return pltpu.with_memory_space_constraint(array, pltpu.HBM)


def dot(a, b, contract=((1,), (0,))):
    return lax.dot_general(a, b, (contract, ((), ())), preferred_element_type=jnp.float32)


def z_order(y_devices):
    order = np.arange(MZ).reshape(y_devices, MZ // y_devices)
    return [np.concatenate([order[d], np.delete(order, d, 0).reshape(-1)]) for d in range(y_devices)]


def z_forward_table(y_devices):
    tables = []
    for kz in z_order(y_devices):
        angle = angles(kz, np.arange(NZ), NZ).T
        parts = np.stack([np.cos(angle), -np.sin(angle)])
        table = np.zeros((2, 2, NZ, 2, 2, MZ))
        for c in range(2):
            for s in range(2):
                table[0, c, :, s, c] = parts[s]
                table[1, c, :, s, c] = parts[1 - s]
        table = halves(table.reshape(2, 2 * NZ, 4 * MZ))
        tables.append(np.concatenate([table[0], table[1]], 2))
    return np.stack(tables)


def stacked(table):
    high, low = halves(table)
    return np.concatenate([np.concatenate([high, high], 1), np.concatenate([low, np.zeros_like(low)], 1)], 0)


def y_forward_table(y_devices):
    tables = []
    rows = NY // y_devices
    for d in range(y_devices):
        angle = angles(kept(NY, MY), d * rows + np.arange(rows), NY)
        table = np.zeros((2, Y_BLOCKS, MP, rows))
        table[0, :, :M] = np.cos(angle).reshape(Y_BLOCKS, M, rows)
        table[1, :, :M] = np.sin(angle).reshape(Y_BLOCKS, M, rows)
        tables.append(stacked(table.reshape(2 * Y_BLOCKS * MP, rows)))
    return np.stack(tables)


def x_table(x_local):
    angle = angles(kept(NX, MX), np.arange(NX).reshape(-1, x_local).T.reshape(-1), NX).T
    table = np.zeros((NX, 2, LANES))
    table[:, 0, :MX] = np.cos(angle)
    table[:, 1, :MX] = np.sin(angle)
    return halves(table.reshape(NX, 2 * LANES))


def y_inverse_table(y_devices):
    tables = []
    rows = NY // y_devices
    for d in range(y_devices):
        angle = angles(kept(NY, MY), d * rows + np.arange(rows), NY).T
        table = np.zeros((2, rows, 2, Y_BLOCKS, MP))
        cosine = np.cos(angle).reshape(rows, Y_BLOCKS, M)
        sine = np.sin(angle).reshape(rows, Y_BLOCKS, M)
        table[0, :, 0, :, :M] = cosine
        table[0, :, 1, :, :M] = -sine
        table[1, :, 0, :, :M] = sine
        table[1, :, 1, :, :M] = cosine
        tables.append(stacked(table.reshape(2 * rows, 2 * Y_BLOCKS * MP)))
    return np.stack(tables)


def z_inverse_table(y_devices):
    tables = []
    for kz in z_order(y_devices):
        angle = angles(kz, np.arange(NZ), NZ)
        weight = np.where(kz == 0, 1.0, 2.0)[:, None] / (NX * NY * NZ)
        parts = np.stack([np.cos(angle) * weight, -np.sin(angle) * weight])
        table = np.zeros((2, 2, 2, MZ, 2, NZ))
        for c in range(2):
            for s in range(2):
                table[0, s, c, :, c] = parts[s]
                table[1, s, c, :, c] = parts[1 - s]
        tables.append(np.swapaxes(halves(table.reshape(2, 4 * MZ, 2 * NZ)), 0, 1))
    return np.stack(tables)


def lane_of_part(shape):
    return lax.broadcasted_iota(jnp.int32, shape, len(shape) - 1) % HALF


def with_spare(row, value, last):
    used = HALF - SPARE
    if row >= used // SPARE:
        return value
    moved = pltpu.roll(last, used - SPARE * row, 1)
    return jnp.where(lane_of_part(value.shape) >= used, moved, value)


def last_row(value_of_row):
    used = HALF - SPARE
    result = value_of_row(0)
    at = lane_of_part(result.shape) // SPARE
    result = pltpu.roll(result, LANES - used, 1)
    for row in range(1, used // SPARE):
        moved = pltpu.roll(value_of_row(row), LANES - used + SPARE * row, 1)
        result = jnp.where(at == row, moved, result)
    return result


def forward_kernel(
    x_local, place, field, z_tables, y_tables, own, other, cells, z_table, y_table, z_hat, rows, loaded
):
    channels, _, y_local, _ = field.shape
    groups = channels // QUAD
    per_x = QUAD * MZ
    half = MZ // 2
    size = Y_BLOCKS * MP
    sent = x_local * QUAD - 1
    order = list(range(x_local))[::-1]
    loads = [pltpu.make_async_copy(field.at[:, x], cells.at[x], loaded.at[x]) for x in range(x_local)]
    tables = [
        pltpu.make_async_copy(z_tables.at[place[0]], z_table, loaded.at[x_local]),
        pltpu.make_async_copy(y_tables.at[place[0]], y_table, loaded.at[x_local + 1]),
    ]
    tables[0].start()
    for x in order[:X_FORWARD]:
        loads[x].start()
    tables[1].start()
    for x in order[X_FORWARD:]:
        loads[x].start()
    last = {}
    for first in range(0, x_local, X_FORWARD):
        chunk = order[first : first + X_FORWARD]
        for x in chunk:
            loads[x].wait()
        if first == 0:
            tables[0].wait()
        for i, x in enumerate(chunk):
            even, odd = (
                dot(
                    jnp.concatenate(
                        [
                            jnp.concatenate([cells[x, QUAD * g + 2 * k], cells[x, QUAD * g + 2 * k + 1]], 1)
                            for g in range(groups)
                        ],
                        0,
                    ),
                    z_table[k],
                )
                for k in range(2)
            )
            even = even[:, :per_x] + even[:, per_x:]
            odd = odd[:, :per_x] + odd[:, per_x:]
            lower = lax.broadcasted_iota(jnp.int32, even.shape, 1) < per_x // 2
            at = pl.ds(i * groups * y_local, groups * y_local)
            z_hat[first // X_FORWARD, at, :per_x] = jnp.where(lower, even, odd)
            z_hat[first // X_FORWARD, at, per_x:] = pltpu.roll(jnp.where(lower, odd, even), per_x // 2, 1)
        if first == 0:
            tables[1].wait()
        for i, x in enumerate(chunk):
            for g in range(groups):
                at = pl.ds((i * groups + g) * y_local, y_local)
                high, low = split(z_hat[first // X_FORWARD, at, :])
                parts = dot(y_table[...], jnp.concatenate([high, low], 0))
                parts = parts[: 2 * size] + parts[2 * size :]
                real = parts[:size, :per_x] + parts[size:, per_x:]
                imag = parts[:size, per_x:] - parts[size:, :per_x]
                for block in range(Y_BLOCKS):
                    for s, value in enumerate((real, imag)):
                        at = pl.ds(s * HALF + g * M, MP)
                        rows[x, block, at, :] = value[block * MP : (block + 1) * MP]
            for block in range(Y_BLOCKS):
                turned = rows[x, block, :LANES, :].T
                for c in reversed(range(QUAD)):
                    row = x * QUAD + c
                    for k, out in enumerate((own, other)):
                        value = turned[c * MZ + k * half : c * MZ + (k + 1) * half]
                        if row == sent:
                            last[block, k] = value
                        else:
                            at = pl.ds(block * sent + row, half, stride=Y_BLOCKS * sent)
                            out[at, :] = with_spare(row, value, last[block, k])


def forward(place, field, y_devices, x_devices):
    channels, x_local, y_local, _ = field.shape
    z_table, y_table = z_forward_table(y_devices), y_forward_table(y_devices)
    payload = jax.ShapeDtypeStruct((x_devices * (x_local * QUAD - 1), LANES), jnp.float32)
    lines = X_FORWARD * (channels // QUAD) * y_local
    vmem = pl.BlockSpec(memory_space=pltpu.VMEM)
    return pl.pallas_call(
        functools.partial(forward_kernel, x_local),
        out_shape=(payload, payload),
        grid_spec=pltpu.PrefetchScalarGridSpec(
            num_scalar_prefetch=1,
            grid=(1,),
            in_specs=[pl.BlockSpec(memory_space=pltpu.HBM)] * 3,
            out_specs=[vmem, vmem],
            scratch_shapes=[
                pltpu.VMEM((x_local, channels, y_local, NZ), field.dtype),
                pltpu.VMEM(z_table.shape[1:], jnp.bfloat16),
                pltpu.VMEM(y_table.shape[1:], jnp.bfloat16),
                pltpu.VMEM((x_local // X_FORWARD, lines, 2 * QUAD * MZ), jnp.float32),
                pltpu.VMEM((x_local, Y_BLOCKS, LANES + MP, LANES), jnp.float32),
                pltpu.SemaphoreType.DMA((x_local + 2,)),
            ],
        ),
        compiler_params=pltpu.CompilerParams(
            dimension_semantics=("arbitrary",), vmem_limit_bytes=24 * MIB
        ),
        name="forward",
    )(place, in_hbm(field), in_hbm(jnp.asarray(z_table)), in_hbm(jnp.asarray(y_table)))


def mix_kernel(x_local, payload_hbm, weights, table_hbm, result, payload, table, spectrum, mixed, done, arrived):
    channels = weights.shape[1]
    sent = x_local * QUAD - 1
    x_devices = payload.shape[0] // sent
    arrival = pltpu.make_async_copy(payload_hbm, payload, arrived)
    arrival.start()
    load = pltpu.make_async_copy(table_hbm, table, done)
    load.start()
    arrival.wait()

    def row_of(row):
        return pl.ds(row, x_devices, stride=sent)

    lines = [payload[row_of(row), :] for row in range(sent)]
    lines.append(last_row(lambda row: lines[row]))
    rows = jnp.concatenate([jnp.concatenate(lines[c::QUAD], 0) for c in range(QUAD)], 1)
    high, low = split(rows.T)
    load.wait()
    parts = dot(high, table[0]) + dot(low, table[0]) + dot(high, table[1])
    for c in range(QUAD):
        upper = parts[c * LANES : c * LANES + HALF]
        lower = parts[c * LANES + HALF : (c + 1) * LANES]
        spectrum[c, 0] = upper[:, :LANES] + lower[:, LANES:]
        spectrum[c, 1] = lower[:, :LANES] - upper[:, LANES:]
    outs = channels // 2
    for first in range(0, channels, outs):
        real = [jnp.zeros((MP, LANES), jnp.float32)] * outs
        imag = [jnp.zeros((MP, LANES), jnp.float32)] * outs
        for i in range(channels):
            g, c = i // QUAD, i % QUAD
            real_in = spectrum[c, 0, pl.ds(g * M, MP), :]
            imag_in = spectrum[c, 1, pl.ds(g * M, MP), :]
            for k in range(outs):
                w_real = weights[0, i, first + k].astype(jnp.float32)
                w_imag = weights[1, i, first + k].astype(jnp.float32)
                real[k] = real[k] + (w_real * real_in - w_imag * imag_in)
                imag[k] = imag[k] + (w_real * imag_in + w_imag * real_in)
        for k in range(outs):
            g, c = (first + k) // QUAD, (first + k) % QUAD
            upper = pl.ds(g * M, MP)
            lower = pl.ds(HALF + g * M, MP)
            mixed[c, upper, :LANES] = real[k]
            mixed[c, upper, LANES:] = -imag[k]
            mixed[c, lower, :LANES] = imag[k]
            mixed[c, lower, LANES:] = real[k]
    last = None
    for c in range(QUAD - 2, -1, -2):
        high, low = split(jnp.concatenate([mixed[c, :LANES, :], mixed[c + 1, :LANES, :]], 0))
        over_k = ((1,), (1,))
        back = dot(table[0], high, over_k) + dot(table[0], low, over_k) + dot(table[1], high, over_k)
        if last is None:
            last = back[(x_local - 1) * x_devices :, LANES:]
        for x in range(x_local):
            for k in range(2):
                row = x * QUAD + c + k
                if row < sent:
                    value = back[x * x_devices : (x + 1) * x_devices, k * LANES : (k + 1) * LANES]
                    result[row_of(row), :] = with_spare(row, value, last)


def mix(payload, weights, x_local):
    table = x_table(x_local)
    vmem = pl.BlockSpec(memory_space=pltpu.VMEM)
    return pl.pallas_call(
        functools.partial(mix_kernel, x_local),
        out_shape=jax.ShapeDtypeStruct(payload.shape, jnp.float32),
        in_specs=[pl.BlockSpec(memory_space=pltpu.HBM), vmem, pl.BlockSpec(memory_space=pltpu.HBM)],
        out_specs=vmem,
        scratch_shapes=[
            pltpu.VMEM(payload.shape, jnp.float32),
            pltpu.VMEM(table.shape, jnp.bfloat16),
            pltpu.VMEM((QUAD, 2, HALF, LANES), jnp.float32),
            pltpu.VMEM((QUAD, LANES + MP, 2 * LANES), jnp.float32),
            pltpu.SemaphoreType.DMA,
            pltpu.SemaphoreType.DMA,
        ],
        compiler_params=pltpu.CompilerParams(vmem_limit_bytes=20 * MIB),
        name="mix",
    )(in_hbm(payload), weights, in_hbm(jnp.asarray(table)))


def pointwise_kernel(field, local, bias, out):
    channels, steps, y_local, _ = field.shape
    for i in range(steps):
        for y in range(0, y_local, 2 * MP):
            pair = [
                field[:, i, y + j * MP : y + (j + 1) * MP, :].reshape(channels * MP, NZ) for j in range(2)
            ]
            mixed = dot(local[...], jnp.concatenate(pair, 1))
            for o in range(channels):
                for j in range(2):
                    value = mixed[o * MP : (o + 1) * MP, j * NZ : (j + 1) * NZ]
                    out[o, i, y + j * MP : y + (j + 1) * MP, :] = value + bias[o]


def pointwise(field, local, bias):
    channels, x_local, y_local, _ = field.shape
    cells = pl.BlockSpec((channels, 1, y_local, NZ), lambda x: (0, x, 0, 0))
    return pl.pallas_call(
        pointwise_kernel,
        out_shape=jax.ShapeDtypeStruct(field.shape, jnp.float32),
        grid=(x_local,),
        in_specs=[cells, pl.BlockSpec(local.shape, lambda x: (0, 0)), pl.BlockSpec(memory_space=pltpu.SMEM)],
        out_specs=cells,
        compiler_params=pltpu.CompilerParams(
            dimension_semantics=("arbitrary",), vmem_limit_bytes=12 * MIB
        ),
        cost_estimate=pl.CostEstimate(
            flops=2 * field.size * channels * MP, transcendentals=0, bytes_accessed=6 * field.size
        ),
        name="pointwise",
    )(field, local, bias)


def inverse_kernel(place, own, other, base, y_table, z_table, out, rows, modes, lines, total, cells, stored):
    del place
    channels, x_local, y_local, _ = base.shape
    groups = channels // QUAD
    half = MZ // 2
    sent = x_local * QUAD - 1
    def row_of(block, row):
        return pl.ds(block * sent + row, half, stride=Y_BLOCKS * sent)

    stores = [pltpu.make_async_copy(cells.at[x], out.at[:, x], stored.at[x]) for x in range(x_local)]
    for first in range(0, x_local, X_INVERSE):
        chunk = range(first, first + X_INVERSE)
        for x in chunk:
            for block in range(Y_BLOCKS):
                for c in range(QUAD):
                    for k, source in enumerate((own, other)):
                        row = x * QUAD + c
                        if row < sent:
                            value = source[row_of(block, row), :]
                        else:
                            value = last_row(lambda r: source[row_of(block, r), :])
                        rows[x, block, c * MZ + k * half : c * MZ + (k + 1) * half] = value
                modes[x, block] = rows[x, block].T
        for g in range(groups):
            inputs = jnp.concatenate(
                [
                    jnp.concatenate([modes[x, block, pl.ds(s * HALF + g * M, MP), :] for x in chunk], 1)
                    for s in range(2)
                    for block in range(Y_BLOCKS)
                ],
                0,
            )
            high, low = split(inputs)
            parts = dot(y_table[0], jnp.concatenate([high, low], 0))
            parts = parts[: 2 * y_local] + parts[2 * y_local :]
            for i in range(X_INVERSE):
                at = pl.ds(((first + i) * groups + g) * y_local, y_local)
                real = parts[:y_local, i * LANES : (i + 1) * LANES]
                imag = pltpu.roll(parts[y_local:, i * LANES : (i + 1) * LANES], LANES // 2, 1)
                lower = lax.broadcasted_iota(jnp.int32, real.shape, 1) < LANES // 2
                for k, value in enumerate((jnp.where(lower, real, imag), jnp.where(lower, imag, real))):
                    high, low = split(value)
                    lines[k, at, :LANES] = high
                    lines[k, at, LANES:] = low
        at = pl.ds(first * groups * y_local, X_INVERSE * groups * y_local)
        for k in range(2):
            high, low = z_table[0, k, 0], z_table[0, k, 1]
            both = dot(lines[k, at, :], jnp.concatenate([high, high], 0))
            total[k, at, :] = both + dot(lines[k, at, :LANES], low)
        scale = math.sqrt(2 / math.pi)
        for x in chunk:
            for o in range(channels):
                g, c = o // QUAD, o % QUAD
                at = pl.ds((x * groups + g) * y_local, y_local)
                value = total[c // 2, at, c % 2 * NZ : (c % 2 + 1) * NZ] + base[o, x]
                inner = value * (scale + (scale * 0.044715) * (value * value))
                scaled = 0.5 * value
                cells[x, o] = (scaled + scaled * jnp.tanh(inner)).astype(out.dtype)
            stores[x].start()
    for store in stores:
        store.wait()


def inverse(place, own, other, base, y_devices, dtype):
    channels, x_local, y_local, _ = base.shape
    z_table, y_table = z_inverse_table(y_devices), y_inverse_table(y_devices)
    vmem = pl.BlockSpec(memory_space=pltpu.VMEM)
    lines = x_local * (channels // QUAD) * y_local
    return pl.pallas_call(
        inverse_kernel,
        out_shape=jax.ShapeDtypeStruct(base.shape, dtype),
        grid_spec=pltpu.PrefetchScalarGridSpec(
            num_scalar_prefetch=1,
            grid=(1,),
            in_specs=[
                vmem,
                vmem,
                vmem,
                pl.BlockSpec((1, *y_table.shape[1:]), lambda x, p: (p[0], 0, 0)),
                pl.BlockSpec((1, *z_table.shape[1:]), lambda x, p: (p[0], 0, 0, 0, 0)),
            ],
            out_specs=pl.BlockSpec(memory_space=pltpu.HBM),
            scratch_shapes=[
                pltpu.VMEM((x_local, Y_BLOCKS, LANES, LANES), jnp.float32),
                pltpu.VMEM((x_local, Y_BLOCKS, LANES, LANES), jnp.float32),
                pltpu.VMEM((2, lines, 2 * LANES), jnp.bfloat16),
                pltpu.VMEM((2, lines, 2 * NZ), jnp.float32),
                pltpu.VMEM((x_local, channels, y_local, NZ), dtype),
                pltpu.SemaphoreType.DMA((x_local,)),
            ],
        ),
        compiler_params=pltpu.CompilerParams(
            dimension_semantics=("arbitrary",), vmem_limit_bytes=36 * MIB
        ),
        name="inverse",
    )(place, own, other, base, jnp.asarray(y_table), jnp.asarray(z_table))


def spread_weights(spectral_weight):
    m, k = spectral_weight.shape[3:]
    return jnp.pad(spectral_weight, ((0, 0), (0, 0), (0, 0), (0, MP - m), (0, LANES - k)))


def local_matrix(pointwise_weight):
    channels = pointwise_weight.shape[0]
    eye = jnp.eye(MP, dtype=pointwise_weight.dtype)
    matrix = pointwise_weight.T[:, None, :, None] * eye[None, :, None, :]
    return matrix.reshape(channels * MP, channels * MP)


def swapped(x, axis):
    devices = lax.axis_size(axis)
    return lax.ppermute(x, axis, [(d, (d + 1) % devices) for d in range(devices)])


def exchanged(rows, axis):
    devices = lax.axis_size(axis)
    blocks = rows.reshape(devices, rows.shape[0] // devices, 1, LANES)
    return lax.all_to_all(blocks, axis, 0, 0, tiled=True).reshape(rows.shape)


def per_device(field, spectral_weight, pointwise_weight, bias):
    y_devices, x_devices = lax.axis_size("py"), lax.axis_size("px")
    place = lax.axis_index("py").astype(jnp.int32).reshape(1)
    cells = field[0]
    own, other = forward(place, cells, y_devices, x_devices)
    payload = own + swapped(other, "py")
    payload, spectral_weight, pointwise_weight, bias = lax.optimization_barrier(
        (payload, spectral_weight, pointwise_weight, bias)
    )
    received = exchanged(payload, "px")
    weights = spread_weights(spectral_weight)
    base = pointwise(cells, local_matrix(pointwise_weight), bias)
    received, base = lax.optimization_barrier((received, base))
    result = mix(received, weights, cells.shape[1])
    own = exchanged(result, "px")
    other = swapped(own, "py")
    return inverse(place, own, other, base, y_devices, field.dtype)[None]


def solution(mesh):
    in_specs = (
        P("groups", None, "px", "py", None),
        P(None, None, None, ("py", "px"), None),
        P(),
        P(),
    )
    out_specs = P("groups", None, "px", "py", None)
    return jax.shard_map(per_device, mesh=mesh, in_specs=in_specs, out_specs=out_specs, check_vma=False)
```

```python
import functools
import math

import jax
import jax.numpy as jnp
import numpy as np
from jax import lax
from jax.experimental import pallas as pl
from jax.experimental.pallas import tpu as pltpu
from jax.sharding import PartitionSpec as P

NX = 384
NY = 192
NZ = 128
MX = 96
MY = 48
MZ = 32

LANES = 128
QUAD = 4
Y_BLOCKS = 4
M = MY // Y_BLOCKS
MP = 16
HALF = 64
SPARE = 4
X_FORWARD = 3
X_INVERSE = 2
MIB = 1024 * 1024


def kept(length, retained):
    index = np.arange(retained)
    return np.where(index < retained // 2, index, length - retained + index)


def angles(frequency, positions, length):
    return 2 * np.pi * ((frequency[:, None] * positions[None, :]) % length) / length


def halves(table):
    high = table.astype(np.float32).astype(jnp.bfloat16)
    low = (table - high.astype(np.float64)).astype(np.float32).astype(jnp.bfloat16)
    return np.stack([high, low])


def split(value):
    high = value.astype(jnp.bfloat16)
    low = (value - high.astype(jnp.float32)).astype(jnp.bfloat16)
    return high, low


def in_hbm(array):
    return pltpu.with_memory_space_constraint(array, pltpu.HBM)


def dot(a, b, contract=((1,), (0,))):
    return lax.dot_general(a, b, (contract, ((), ())), preferred_element_type=jnp.float32)


def z_order(y_devices):
    order = np.arange(MZ).reshape(y_devices, MZ // y_devices)
    return [np.concatenate([order[d], np.delete(order, d, 0).reshape(-1)]) for d in range(y_devices)]


def z_forward_table(y_devices):
    tables = []
    for kz in z_order(y_devices):
        angle = angles(kz, np.arange(NZ), NZ).T
        parts = np.stack([np.cos(angle), -np.sin(angle)])
        table = np.zeros((2, 2, NZ, 2, 2, MZ))
        for c in range(2):
            for s in range(2):
                table[0, c, :, s, c] = parts[s]
                table[1, c, :, s, c] = parts[1 - s]
        table = halves(table.reshape(2, 2 * NZ, 4 * MZ))
        tables.append(np.concatenate([table[0], table[1]], 2))
    return np.stack(tables)


def stacked(table):
    high, low = halves(table)
    return np.concatenate([np.concatenate([high, high], 1), np.concatenate([low, np.zeros_like(low)], 1)], 0)


def y_forward_table(y_devices):
    tables = []
    rows = NY // y_devices
    for d in range(y_devices):
        angle = angles(kept(NY, MY), d * rows + np.arange(rows), NY)
        table = np.zeros((2, Y_BLOCKS, MP, rows))
        table[0, :, :M] = np.cos(angle).reshape(Y_BLOCKS, M, rows)
        table[1, :, :M] = np.sin(angle).reshape(Y_BLOCKS, M, rows)
        tables.append(stacked(table.reshape(2 * Y_BLOCKS * MP, rows)))
    return np.stack(tables)


def x_table(x_local):
    angle = angles(kept(NX, MX), np.arange(NX).reshape(-1, x_local).T.reshape(-1), NX).T
    table = np.zeros((NX, 2, LANES))
    table[:, 0, :MX] = np.cos(angle)
    table[:, 1, :MX] = np.sin(angle)
    return halves(table.reshape(NX, 2 * LANES))


def y_inverse_table(y_devices):
    tables = []
    rows = NY // y_devices
    for d in range(y_devices):
        angle = angles(kept(NY, MY), d * rows + np.arange(rows), NY).T
        table = np.zeros((2, rows, 2, Y_BLOCKS, MP))
        cosine = np.cos(angle).reshape(rows, Y_BLOCKS, M)
        sine = np.sin(angle).reshape(rows, Y_BLOCKS, M)
        table[0, :, 0, :, :M] = cosine
        table[0, :, 1, :, :M] = -sine
        table[1, :, 0, :, :M] = sine
        table[1, :, 1, :, :M] = cosine
        tables.append(stacked(table.reshape(2 * rows, 2 * Y_BLOCKS * MP)))
    return np.stack(tables)


def z_inverse_table(y_devices):
    tables = []
    for kz in z_order(y_devices):
        angle = angles(kz, np.arange(NZ), NZ)
        weight = np.where(kz == 0, 1.0, 2.0)[:, None] / (NX * NY * NZ)
        parts = np.stack([np.cos(angle) * weight, -np.sin(angle) * weight])
        table = np.zeros((2, 2, 2, MZ, 2, NZ))
        for c in range(2):
            for s in range(2):
                table[0, s, c, :, c] = parts[s]
                table[1, s, c, :, c] = parts[1 - s]
        tables.append(np.swapaxes(halves(table.reshape(2, 4 * MZ, 2 * NZ)), 0, 1))
    return np.stack(tables)


def lane_of_part(shape):
    return lax.broadcasted_iota(jnp.int32, shape, len(shape) - 1) % HALF


def with_spare(row, value, last):
    used = HALF - SPARE
    if row >= used // SPARE:
        return value
    moved = pltpu.roll(last, used - SPARE * row, 1)
    return jnp.where(lane_of_part(value.shape) >= used, moved, value)


def last_row(value_of_row):
    used = HALF - SPARE
    result = value_of_row(0)
    at = lane_of_part(result.shape) // SPARE
    result = pltpu.roll(result, LANES - used, 1)
    for row in range(1, used // SPARE):
        moved = pltpu.roll(value_of_row(row), LANES - used + SPARE * row, 1)
        result = jnp.where(at == row, moved, result)
    return result


def forward_kernel(
    x_local, place, field, z_tables, y_tables, own, other, cells, z_table, y_table, z_hat, rows, loaded
):
    channels, _, y_local, _ = field.shape
    groups = channels // QUAD
    per_x = QUAD * MZ
    half = MZ // 2
    size = Y_BLOCKS * MP
    sent = x_local * QUAD - 1
    order = list(range(x_local))[::-1]
    loads = [pltpu.make_async_copy(field.at[:, x], cells.at[x], loaded.at[x]) for x in range(x_local)]
    tables = [
        pltpu.make_async_copy(z_tables.at[place[0]], z_table, loaded.at[x_local]),
        pltpu.make_async_copy(y_tables.at[place[0]], y_table, loaded.at[x_local + 1]),
    ]
    tables[0].start()
    for x in order[:X_FORWARD]:
        loads[x].start()
    tables[1].start()
    for x in order[X_FORWARD:]:
        loads[x].start()
    last = {}
    for first in range(0, x_local, X_FORWARD):
        chunk = order[first : first + X_FORWARD]
        for x in chunk:
            loads[x].wait()
        if first == 0:
            tables[0].wait()
        for i, x in enumerate(chunk):
            even, odd = (
                dot(
                    jnp.concatenate(
                        [
                            jnp.concatenate([cells[x, QUAD * g + 2 * k], cells[x, QUAD * g + 2 * k + 1]], 1)
                            for g in range(groups)
                        ],
                        0,
                    ),
                    z_table[k],
                )
                for k in range(2)
            )
            even = even[:, :per_x] + even[:, per_x:]
            odd = odd[:, :per_x] + odd[:, per_x:]
            lower = lax.broadcasted_iota(jnp.int32, even.shape, 1) < per_x // 2
            at = pl.ds(i * groups * y_local, groups * y_local)
            z_hat[first // X_FORWARD, at, :per_x] = jnp.where(lower, even, odd)
            z_hat[first // X_FORWARD, at, per_x:] = pltpu.roll(jnp.where(lower, odd, even), per_x // 2, 1)
        if first == 0:
            tables[1].wait()
        for i, x in enumerate(chunk):
            for g in range(groups):
                at = pl.ds((i * groups + g) * y_local, y_local)
                high, low = split(z_hat[first // X_FORWARD, at, :])
                parts = dot(y_table[...], jnp.concatenate([high, low], 0))
                parts = parts[: 2 * size] + parts[2 * size :]
                real = parts[:size, :per_x] + parts[size:, per_x:]
                imag = parts[:size, per_x:] - parts[size:, :per_x]
                for block in range(Y_BLOCKS):
                    for s, value in enumerate((real, imag)):
                        at = pl.ds(s * HALF + g * M, MP)
                        rows[x, block, at, :] = value[block * MP : (block + 1) * MP]
            for block in range(Y_BLOCKS):
                turned = rows[x, block, :LANES, :].T
                for c in reversed(range(QUAD)):
                    row = x * QUAD + c
                    for k, out in enumerate((own, other)):
                        value = turned[c * MZ + k * half : c * MZ + (k + 1) * half]
                        if row == sent:
                            last[block, k] = value
                        else:
                            at = pl.ds(block * sent + row, half, stride=Y_BLOCKS * sent)
                            out[at, :] = with_spare(row, value, last[block, k])


def forward(place, field, y_devices, x_devices):
    channels, x_local, y_local, _ = field.shape
    z_table, y_table = z_forward_table(y_devices), y_forward_table(y_devices)
    payload = jax.ShapeDtypeStruct((x_devices * (x_local * QUAD - 1), LANES), jnp.float32)
    lines = X_FORWARD * (channels // QUAD) * y_local
    vmem = pl.BlockSpec(memory_space=pltpu.VMEM)
    return pl.pallas_call(
        functools.partial(forward_kernel, x_local),
        out_shape=(payload, payload),
        grid_spec=pltpu.PrefetchScalarGridSpec(
            num_scalar_prefetch=1,
            grid=(1,),
            in_specs=[pl.BlockSpec(memory_space=pltpu.HBM)] * 3,
            out_specs=[vmem, vmem],
            scratch_shapes=[
                pltpu.VMEM((x_local, channels, y_local, NZ), field.dtype),
                pltpu.VMEM(z_table.shape[1:], jnp.bfloat16),
                pltpu.VMEM(y_table.shape[1:], jnp.bfloat16),
                pltpu.VMEM((x_local // X_FORWARD, lines, 2 * QUAD * MZ), jnp.float32),
                pltpu.VMEM((x_local, Y_BLOCKS, LANES + MP, LANES), jnp.float32),
                pltpu.SemaphoreType.DMA((x_local + 2,)),
            ],
        ),
        compiler_params=pltpu.CompilerParams(
            dimension_semantics=("arbitrary",), vmem_limit_bytes=24 * MIB
        ),
        name="forward",
    )(place, in_hbm(field), in_hbm(jnp.asarray(z_table)), in_hbm(jnp.asarray(y_table)))


def mix_kernel(x_local, payload_hbm, weights, table_hbm, result, payload, table, spectrum, mixed, done, arrived):
    channels = weights.shape[1]
    sent = x_local * QUAD - 1
    x_devices = payload.shape[0] // sent
    arrival = pltpu.make_async_copy(payload_hbm, payload, arrived)
    arrival.start()
    load = pltpu.make_async_copy(table_hbm, table, done)
    load.start()
    arrival.wait()

    def row_of(row):
        return pl.ds(row, x_devices, stride=sent)

    lines = [payload[row_of(row), :] for row in range(sent)]
    lines.append(last_row(lambda row: lines[row]))
    rows = jnp.concatenate([jnp.concatenate(lines[c::QUAD], 0) for c in range(QUAD)], 1)
    high, low = split(rows.T)
    load.wait()
    parts = dot(high, table[0]) + dot(low, table[0]) + dot(high, table[1])
    for c in range(QUAD):
        upper = parts[c * LANES : c * LANES + HALF]
        lower = parts[c * LANES + HALF : (c + 1) * LANES]
        spectrum[c, 0] = upper[:, :LANES] + lower[:, LANES:]
        spectrum[c, 1] = lower[:, :LANES] - upper[:, LANES:]
    outs = channels // 2
    for first in range(0, channels, outs):
        real = [jnp.zeros((MP, LANES), jnp.float32)] * outs
        imag = [jnp.zeros((MP, LANES), jnp.float32)] * outs
        for i in range(channels):
            g, c = i // QUAD, i % QUAD
            real_in = spectrum[c, 0, pl.ds(g * M, MP), :]
            imag_in = spectrum[c, 1, pl.ds(g * M, MP), :]
            for k in range(outs):
                w_real = weights[0, i, first + k].astype(jnp.float32)
                w_imag = weights[1, i, first + k].astype(jnp.float32)
                real[k] = real[k] + (w_real * real_in - w_imag * imag_in)
                imag[k] = imag[k] + (w_real * imag_in + w_imag * real_in)
        for k in range(outs):
            g, c = (first + k) // QUAD, (first + k) % QUAD
            upper = pl.ds(g * M, MP)
            lower = pl.ds(HALF + g * M, MP)
            mixed[c, upper, :LANES] = real[k]
            mixed[c, upper, LANES:] = -imag[k]
            mixed[c, lower, :LANES] = imag[k]
            mixed[c, lower, LANES:] = real[k]
    last = None
    for c in range(QUAD - 2, -1, -2):
        high, low = split(jnp.concatenate([mixed[c, :LANES, :], mixed[c + 1, :LANES, :]], 0))
        over_k = ((1,), (1,))
        back = dot(table[0], high, over_k) + dot(table[0], low, over_k) + dot(table[1], high, over_k)
        if last is None:
            last = back[(x_local - 1) * x_devices :, LANES:]
        for x in range(x_local):
            for k in range(2):
                row = x * QUAD + c + k
                if row < sent:
                    value = back[x * x_devices : (x + 1) * x_devices, k * LANES : (k + 1) * LANES]
                    result[row_of(row), :] = with_spare(row, value, last)


def mix(payload, weights, x_local):
    table = x_table(x_local)
    vmem = pl.BlockSpec(memory_space=pltpu.VMEM)
    return pl.pallas_call(
        functools.partial(mix_kernel, x_local),
        out_shape=jax.ShapeDtypeStruct(payload.shape, jnp.float32),
        in_specs=[pl.BlockSpec(memory_space=pltpu.HBM), vmem, pl.BlockSpec(memory_space=pltpu.HBM)],
        out_specs=vmem,
        scratch_shapes=[
            pltpu.VMEM(payload.shape, jnp.float32),
            pltpu.VMEM(table.shape, jnp.bfloat16),
            pltpu.VMEM((QUAD, 2, HALF, LANES), jnp.float32),
            pltpu.VMEM((QUAD, LANES + MP, 2 * LANES), jnp.float32),
            pltpu.SemaphoreType.DMA,
            pltpu.SemaphoreType.DMA,
        ],
        compiler_params=pltpu.CompilerParams(vmem_limit_bytes=20 * MIB),
        name="mix",
    )(in_hbm(payload), weights, in_hbm(jnp.asarray(table)))


def pointwise_kernel(field, local, bias, out):
    channels, steps, y_local, _ = field.shape
    for i in range(steps):
        for y in range(0, y_local, 2 * MP):
            pair = [
                field[:, i, y + j * MP : y + (j + 1) * MP, :].reshape(channels * MP, NZ) for j in range(2)
            ]
            mixed = dot(local[...], jnp.concatenate(pair, 1))
            for o in range(channels):
                for j in range(2):
                    value = mixed[o * MP : (o + 1) * MP, j * NZ : (j + 1) * NZ]
                    out[o, i, y + j * MP : y + (j + 1) * MP, :] = value + bias[o]


def pointwise(field, local, bias):
    channels, x_local, y_local, _ = field.shape
    cells = pl.BlockSpec((channels, 1, y_local, NZ), lambda x: (0, x, 0, 0))
    return pl.pallas_call(
        pointwise_kernel,
        out_shape=jax.ShapeDtypeStruct(field.shape, jnp.float32),
        grid=(x_local,),
        in_specs=[cells, pl.BlockSpec(local.shape, lambda x: (0, 0)), pl.BlockSpec(memory_space=pltpu.SMEM)],
        out_specs=cells,
        compiler_params=pltpu.CompilerParams(
            dimension_semantics=("arbitrary",), vmem_limit_bytes=12 * MIB
        ),
        cost_estimate=pl.CostEstimate(
            flops=2 * field.size * channels * MP, transcendentals=0, bytes_accessed=6 * field.size
        ),
        name="pointwise",
    )(field, local, bias)


def inverse_kernel(
    place, own, other, base, y_table, z_tables, out, z_table, rows, modes, lines, total, cells, stored, loaded
):
    load = pltpu.make_async_copy(z_tables.at[place[0]], z_table, loaded)
    load.start()
    channels, x_local, y_local, _ = base.shape
    groups = channels // QUAD
    half = MZ // 2
    sent = x_local * QUAD - 1
    def row_of(block, row):
        return pl.ds(block * sent + row, half, stride=Y_BLOCKS * sent)

    stores = [pltpu.make_async_copy(cells.at[x], out.at[:, x], stored.at[x]) for x in range(x_local)]
    for first in range(0, x_local, X_INVERSE):
        chunk = range(first, first + X_INVERSE)
        for x in chunk:
            for block in range(Y_BLOCKS):
                for c in range(QUAD):
                    for k, source in enumerate((own, other)):
                        row = x * QUAD + c
                        if row < sent:
                            value = source[row_of(block, row), :]
                        else:
                            value = last_row(lambda r: source[row_of(block, r), :])
                        rows[x, block, c * MZ + k * half : c * MZ + (k + 1) * half] = value
                modes[x, block] = rows[x, block].T
        for g in range(groups):
            inputs = jnp.concatenate(
                [
                    jnp.concatenate([modes[x, block, pl.ds(s * HALF + g * M, MP), :] for x in chunk], 1)
                    for s in range(2)
                    for block in range(Y_BLOCKS)
                ],
                0,
            )
            high, low = split(inputs)
            parts = dot(y_table[0], jnp.concatenate([high, low], 0))
            parts = parts[: 2 * y_local] + parts[2 * y_local :]
            for i in range(X_INVERSE):
                at = pl.ds(((first + i) * groups + g) * y_local, y_local)
                real = parts[:y_local, i * LANES : (i + 1) * LANES]
                imag = pltpu.roll(parts[y_local:, i * LANES : (i + 1) * LANES], LANES // 2, 1)
                lower = lax.broadcasted_iota(jnp.int32, real.shape, 1) < LANES // 2
                for k, value in enumerate((jnp.where(lower, real, imag), jnp.where(lower, imag, real))):
                    high, low = split(value)
                    lines[k, at, :LANES] = high
                    lines[k, at, LANES:] = low
        at = pl.ds(first * groups * y_local, X_INVERSE * groups * y_local)
        if first == 0:
            load.wait()
        for k in range(2):
            high, low = z_table[k, 0], z_table[k, 1]
            both = dot(lines[k, at, :], jnp.concatenate([high, high], 0))
            total[k, at, :] = both + dot(lines[k, at, :LANES], low)
        scale = math.sqrt(2 / math.pi)
        for x in chunk:
            for o in range(channels):
                g, c = o // QUAD, o % QUAD
                at = pl.ds((x * groups + g) * y_local, y_local)
                value = total[c // 2, at, c % 2 * NZ : (c % 2 + 1) * NZ] + base[o, x]
                inner = value * (scale + (scale * 0.044715) * (value * value))
                scaled = 0.5 * value
                cells[x, o] = (scaled + scaled * jnp.tanh(inner)).astype(out.dtype)
            stores[x].start()
    for store in stores:
        store.wait()


def inverse(place, own, other, base, y_devices, dtype):
    channels, x_local, y_local, _ = base.shape
    z_table, y_table = z_inverse_table(y_devices), y_inverse_table(y_devices)
    vmem = pl.BlockSpec(memory_space=pltpu.VMEM)
    lines = x_local * (channels // QUAD) * y_local
    return pl.pallas_call(
        inverse_kernel,
        out_shape=jax.ShapeDtypeStruct(base.shape, dtype),
        grid_spec=pltpu.PrefetchScalarGridSpec(
            num_scalar_prefetch=1,
            grid=(1,),
            in_specs=[
                vmem,
                vmem,
                vmem,
                pl.BlockSpec((1, *y_table.shape[1:]), lambda x, p: (p[0], 0, 0)),
                pl.BlockSpec(memory_space=pltpu.HBM),
            ],
            out_specs=pl.BlockSpec(memory_space=pltpu.HBM),
            scratch_shapes=[
                pltpu.VMEM(z_table.shape[1:], jnp.bfloat16),
                pltpu.VMEM((x_local, Y_BLOCKS, LANES, LANES), jnp.float32),
                pltpu.VMEM((x_local, Y_BLOCKS, LANES, LANES), jnp.float32),
                pltpu.VMEM((2, lines, 2 * LANES), jnp.bfloat16),
                pltpu.VMEM((2, lines, 2 * NZ), jnp.float32),
                pltpu.VMEM((x_local, channels, y_local, NZ), dtype),
                pltpu.SemaphoreType.DMA((x_local,)),
                pltpu.SemaphoreType.DMA,
            ],
        ),
        compiler_params=pltpu.CompilerParams(
            dimension_semantics=("arbitrary",), vmem_limit_bytes=36 * MIB
        ),
        name="inverse",
    )(place, own, other, base, jnp.asarray(y_table), in_hbm(jnp.asarray(z_table)))


def spread_weights(spectral_weight):
    m, k = spectral_weight.shape[3:]
    return jnp.pad(spectral_weight, ((0, 0), (0, 0), (0, 0), (0, MP - m), (0, LANES - k)))


def local_matrix(pointwise_weight):
    channels = pointwise_weight.shape[0]
    eye = jnp.eye(MP, dtype=pointwise_weight.dtype)
    matrix = pointwise_weight.T[:, None, :, None] * eye[None, :, None, :]
    return matrix.reshape(channels * MP, channels * MP)


def swapped(x, axis):
    devices = lax.axis_size(axis)
    return lax.ppermute(x, axis, [(d, (d + 1) % devices) for d in range(devices)])


def exchanged(rows, axis):
    devices = lax.axis_size(axis)
    blocks = rows.reshape(devices, rows.shape[0] // devices, 1, LANES)
    return lax.all_to_all(blocks, axis, 0, 0, tiled=True).reshape(rows.shape)


def per_device(field, spectral_weight, pointwise_weight, bias):
    y_devices, x_devices = lax.axis_size("py"), lax.axis_size("px")
    place = lax.axis_index("py").astype(jnp.int32).reshape(1)
    cells = field[0]
    own, other = forward(place, cells, y_devices, x_devices)
    payload = own + swapped(other, "py")
    payload, spectral_weight, pointwise_weight, bias = lax.optimization_barrier(
        (payload, spectral_weight, pointwise_weight, bias)
    )
    received = exchanged(payload, "px")
    weights = spread_weights(spectral_weight)
    base = pointwise(cells, local_matrix(pointwise_weight), bias)
    received, base = lax.optimization_barrier((received, base))
    result = mix(received, weights, cells.shape[1])
    own = exchanged(result, "px")
    other = swapped(own, "py")
    return inverse(place, own, other, base, y_devices, field.dtype)[None]


def solution(mesh):
    in_specs = (
        P("groups", None, "px", "py", None),
        P(None, None, None, ("py", "px"), None),
        P(),
        P(),
    )
    out_specs = P("groups", None, "px", "py", None)
    return jax.shard_map(per_device, mesh=mesh, in_specs=in_specs, out_specs=out_specs, check_vma=False)
```
